128 devices in a mesh: batch: 1, outer: 2 (over core), rows: 64 (over z, y, x).
Axes of the slice: x: 4, y: 4, z: 4, core: 2. Of those that a mesh axis runs over, the one named last changes fastest.
Arguments:
- a_mat: float32 [131072, 1024], P(('batch', 'outer', 'rows'))
Outputs:
- output 1: float32 [131072, 1024], P(('batch', 'outer', 'rows'))
- output 2: float32 [1024, 1024], P('batch')
All inputs are finite; a program needn't handle non-finite values.
Results may differ from the reference program's by a relative error of at most 0.001.
Values sent between devices are 32-bit elements.
A program may use at most 1 GiB of HBM per device.

```python
import math
import jax
import jax.numpy as jnp
from jax import lax

N = 1024
ROWS_DEV = 1024
SHARDS = 128
COND = 300
TOTAL_ROWS = ROWS_DEV * SHARDS
PRECISION = lax.Precision.HIGHEST


def setup_inputs(seed: int = 0, part: int = 0) -> dict:
    part_key = jax.random.fold_in(jax.random.key(seed), part)
    key_rows, key_mix = jax.random.split(part_key)
    gauss_draw = jax.random.normal(key_rows, (SHARDS, ROWS_DEV, N), jnp.float32)
    col_owner = jnp.arange(N) % SHARDS
    boosted = col_owner[None, :] == jnp.arange(SHARDS)[:, None]
    col_weight = jnp.where(boosted, 2.0 * math.sqrt(SHARDS), 1.0) * math.sqrt(SHARDS / (5.0 * SHARDS - 1.0))
    base_rows = (gauss_draw * col_weight[:, None, :]).reshape(TOTAL_ROWS, N)
    spectrum = jnp.power(float(COND), -jnp.arange(N).astype(jnp.float32) / (N - 1))
    mix_basis = jnp.linalg.qr(jax.random.normal(key_mix, (N, N), jnp.float32))[0]
    a_mat = jnp.dot(base_rows * spectrum[None, :], mix_basis.T, precision=PRECISION, preferred_element_type=jnp.float32)
    return {"a_mat": a_mat.astype(jnp.float32)}


def gram_of(block):
    return lax.dot_general(block, block, (((0,), (0,)), ((), ())), precision=PRECISION, preferred_element_type=jnp.float32)


def reference(a_mat):
    chol_one = jnp.linalg.cholesky(gram_of(a_mat))
    q_first = lax.linalg.triangular_solve(chol_one, a_mat, left_side=False, lower=True, transpose_a=True)
    chol_two = jnp.linalg.cholesky(gram_of(q_first))
    q_mat = lax.linalg.triangular_solve(chol_two, q_first, left_side=False, lower=True, transpose_a=True)
    r_mat = lax.dot_general(chol_two, chol_one, (((0,), (1,)), ((), ())), precision=PRECISION, preferred_element_type=jnp.float32)
    return (q_mat, r_mat)
```

```python
import jax
import jax.numpy as jnp
from jax import lax
from jax.experimental import pallas as pl
from jax.experimental.pallas import tpu as pltpu
from jax.sharding import PartitionSpec as P

GROUP_AXES = ("outer", "rows")
HI = lax.Precision.HIGHEST
N = 1024
NB = 128
SUB = 8


def mm(a, b):
    return lax.dot_general(a, b, (((1,), (0,)), ((), ())), precision=HI, preferred_element_type=jnp.float32)


def mm_tn(a, b):
    return lax.dot_general(a, b, (((0,), (0,)), ((), ())), precision=HI, preferred_element_type=jnp.float32)


def mm_nt(a, b):
    return lax.dot_general(a, b, (((1,), (1,)), ((), ())), precision=HI, preferred_element_type=jnp.float32)


def lane(v, c):
    return jnp.broadcast_to(v[:, c:c + 1], (SUB, NB))


def factor_diag(s_ref):
    groups = NB // SUB
    for g in range(groups):
        base = SUB * g
        t = []
        for i in range(SUB):
            t.append([jnp.broadcast_to(s_ref[base + i:base + i + 1, h * NB:(h + 1) * NB], (SUB, NB)) for h in range(2)])
        a = {}
        for i in range(SUB):
            for j in range(i, SUB):
                a[i, j] = lane(t[i][0], base + j)
        inv = []
        u = {}
        rows = []
        for j in range(SUB):
            rs = lax.rsqrt(a[j, j])
            inv.append(rs)
            for i in range(j + 1, SUB):
                u[j, i] = a[j, i] * rs
            for i in range(j + 1, SUB):
                for i2 in range(i, SUB):
                    a[i, i2] = a[i, i2] - u[j, i] * u[j, i2]
            row = [t[j][h] * rs for h in range(2)]
            rows.append(row)
            for i in range(j + 1, SUB):
                for h in range(2):
                    t[i][h] = t[i][h] - u[j, i] * row[h]
        for j in range(SUB):
            for h in range(2):
                s_ref[base + j:base + j + 1, h * NB:(h + 1) * NB] = rows[j][h][0:1, :]
        for r in range(g + 1, groups):
            blk = [s_ref[SUB * r:SUB * r + SUB, h * NB:(h + 1) * NB] for h in range(2)]
            v = [lane(blk[0], base + j) for j in range(SUB)]
            for j in range(SUB):
                m = v[j] * inv[j]
                for j2 in range(j + 1, SUB):
                    v[j2] = v[j2] - m * u[j, j2]
                for h in range(2):
                    blk[h] = blk[h] - m * rows[j][h]
            for h in range(2):
                s_ref[SUB * r:SUB * r + SUB, h * NB:(h + 1) * NB] = blk[h]


PB = 256
NP = N // PB


def ds(i, n):
    return pl.ds(pl.multiple_of(i * n, n), n)


def loop(lo, hi, body):
    def step(i, carry):
        body(i)
        return carry
    lax.fori_loop(lo, hi, step, 0)


def tri_iota():
    r = lax.broadcasted_iota(jnp.int32, (NB, NB), 0)
    c = lax.broadcasted_iota(jnp.int32, (NB, NB), 1)
    return r, c


def sweep_body(w_ref, q_ref, s_ref, inv_ref):
    r, c = tri_iota()

    def panel(p):
        def half(h):
            k = 2 * p + h
            rows = ds(k, NB)
            s_ref[:, :NB] = w_ref[rows, rows]
            s_ref[:, NB:] = jnp.where(r == c, 1.0, 0.0).astype(jnp.float32)
            factor_diag(s_ref)
            w_ref[rows, rows] = jnp.where(c >= r, s_ref[:, :NB], 0.0)
            li = s_ref[:, NB:]
            inv_ref[pl.ds(pl.multiple_of(h * NB, NB), NB), pl.ds(pl.multiple_of(h * NB, NB), NB)] = li
            loop(k + 1, N // NB, lambda j: w_ref.__setitem__((rows, ds(j, NB)), mm(li, w_ref[rows, ds(j, NB)])))

            @pl.when(h == 0)
            def _():
                nxt = ds(k + 1, NB)
                lhs = w_ref[rows, nxt]
                def upd(j):
                    w_ref[nxt, ds(j, NB)] = w_ref[nxt, ds(j, NB)] - mm_tn(lhs, w_ref[rows, ds(j, NB)])
                loop(k + 1, N // NB, upd)

        loop(0, 2, half)
        pr = ds(p, PB)
        i0 = inv_ref[:NB, :NB]
        i1 = inv_ref[NB:, NB:]
        u01 = w_ref[ds(2 * p, NB), ds(2 * p + 1, NB)]
        inv_ref[NB:, :NB] = -mm(i1, mm_tn(u01, i0))
        inv_ref[:NB, NB:] = jnp.zeros((NB, NB), jnp.float32)

        def trail(i):
            def cols(j):
                w_ref[ds(i, PB), ds(j, PB)] = w_ref[ds(i, PB), ds(j, PB)] - mm_tn(w_ref[pr, ds(i, PB)], w_ref[pr, ds(j, PB)])
            loop(i, NP, cols)
        loop(p + 1, NP, trail)

        def chunk(m):
            rr = ds(m, PB)
            def prev(t):
                q_ref[rr, pr] = q_ref[rr, pr] - mm(q_ref[rr, ds(t, PB)], w_ref[ds(t, PB), pr])
            loop(0, p, prev)
            q_ref[rr, pr] = mm_nt(q_ref[rr, pr], inv_ref[...])
        loop(0, N // PB, chunk)

    loop(0, NP, panel)

    def zero(k):
        def zz(j):
            w_ref[ds(k, NB), ds(j, NB)] = jnp.zeros((NB, NB), jnp.float32)
        loop(0, k, zz)
    loop(1, N // NB, zero)


def tri_index(i, j):
    return i * NP - (i * (i - 1)) // 2 + j - i


NTRI = NP * (NP + 1) // 2


def gram_kernel(a_ref, g_ref):
    def bi(i):
        def bj(j):
            g_ref[tri_index(i, j)] = mm_tn(a_ref[:, ds(i, PB)], a_ref[:, ds(j, PB)])
        loop(i, NP, bj)
    loop(0, NP, bi)


def unpack(g_ref, u_ref):
    for i in range(NP):
        for j in range(i, NP):
            u_ref[i * PB:(i + 1) * PB, j * PB:(j + 1) * PB] = g_ref[tri_index(i, j)]


def first_kernel(g_ref, b_ref, u_ref, q_ref, s_ref, inv_ref):
    unpack(g_ref, u_ref)
    q_ref[...] = b_ref[...]
    sweep_body(u_ref, q_ref, s_ref, inv_ref)


def second_kernel(g_ref, b_ref, u1_ref, r_ref, q_ref, u_ref, s_ref, inv_ref):
    unpack(g_ref, u_ref)
    q_ref[...] = b_ref[...]
    sweep_body(u_ref, q_ref, s_ref, inv_ref)
    r_ref[...] = jnp.zeros((N, N), jnp.float32)

    def ri(i):
        def rj(j):
            def rk(k):
                r_ref[ds(i, PB), ds(j, PB)] = r_ref[ds(i, PB), ds(j, PB)] + mm(u_ref[ds(i, PB), ds(k, PB)], u1_ref[ds(k, PB), ds(j, PB)])
            loop(i, j + 1, rk)
        loop(i, NP, rj)
    loop(0, NP, ri)


VM = pl.BlockSpec(memory_space=pltpu.VMEM)
SQ = jax.ShapeDtypeStruct((N, N), jnp.float32)
PARAMS = pltpu.CompilerParams(vmem_limit_bytes=60 * 1024 * 1024)
WORK = [pltpu.VMEM((NB, 2 * NB), jnp.float32), pltpu.VMEM((PB, PB), jnp.float32)]


def gram(a):
    return pl.pallas_call(gram_kernel, out_shape=jax.ShapeDtypeStruct((NTRI, PB, PB), jnp.float32), in_specs=[VM], out_specs=VM, compiler_params=PARAMS)(a)


def first_sweep(g, a):
    return pl.pallas_call(first_kernel, out_shape=[SQ, SQ], in_specs=[VM] * 2, out_specs=[VM] * 2, scratch_shapes=WORK, compiler_params=PARAMS)(g, a)


def second_sweep(g, q, u1):
    return pl.pallas_call(second_kernel, out_shape=[SQ, SQ], in_specs=[VM] * 3, out_specs=[VM] * 2, scratch_shapes=[pltpu.VMEM((N, N), jnp.float32)] + WORK, compiler_params=PARAMS)(g, q, u1)


def solution(mesh):
    row_spec = P(("batch", "outer", "rows"), None)

    def group_qr(a_block):
        u1, q1 = first_sweep(lax.psum(gram(a_block), GROUP_AXES), a_block)
        r_block, q_block = second_sweep(lax.psum(gram(q1), GROUP_AXES), q1, u1)
        return q_block, r_block

    return jax.shard_map(group_qr, mesh=mesh, in_specs=(row_spec,), out_specs=(row_spec, P("batch", None)), check_vma=False)
```

```python
import jax
import jax.numpy as jnp
from jax import lax
from jax.experimental import pallas as pl
from jax.experimental.pallas import tpu as pltpu
from jax.sharding import PartitionSpec as P

HI = lax.Precision.HIGHEST
N = 1024
NB = 128
SUB = 8


def mm(a, b):
    return lax.dot_general(a, b, (((1,), (0,)), ((), ())), precision=HI, preferred_element_type=jnp.float32)


def mm_tn(a, b):
    return lax.dot_general(a, b, (((0,), (0,)), ((), ())), precision=HI, preferred_element_type=jnp.float32)


def mm_nt(a, b):
    return lax.dot_general(a, b, (((1,), (1,)), ((), ())), precision=HI, preferred_element_type=jnp.float32)


def lane(v, c):
    return jnp.broadcast_to(v[:, c:c + 1], (SUB, NB))


def factor_diag(s_ref):
    groups = NB // SUB
    for g in range(groups):
        base = SUB * g
        t = []
        for i in range(SUB):
            t.append([jnp.broadcast_to(s_ref[base + i:base + i + 1, h * NB:(h + 1) * NB], (SUB, NB)) for h in range(2)])
        a = {}
        for i in range(SUB):
            for j in range(i, SUB):
                a[i, j] = lane(t[i][0], base + j)
        inv = []
        u = {}
        rows = []
        for j in range(SUB):
            rs = lax.rsqrt(a[j, j])
            inv.append(rs)
            for i in range(j + 1, SUB):
                u[j, i] = a[j, i] * rs
            for i in range(j + 1, SUB):
                for i2 in range(i, SUB):
                    a[i, i2] = a[i, i2] - u[j, i] * u[j, i2]
            row = [t[j][h] * rs for h in range(2)]
            rows.append(row)
            for i in range(j + 1, SUB):
                for h in range(2):
                    t[i][h] = t[i][h] - u[j, i] * row[h]
        for j in range(SUB):
            for h in range(2):
                s_ref[base + j:base + j + 1, h * NB:(h + 1) * NB] = rows[j][h][0:1, :]
        for r in range(g + 1, groups):
            blk = [s_ref[SUB * r:SUB * r + SUB, h * NB:(h + 1) * NB] for h in range(2)]
            v = [lane(blk[0], base + j) for j in range(SUB)]
            for j in range(SUB):
                m = v[j] * inv[j]
                for j2 in range(j + 1, SUB):
                    v[j2] = v[j2] - m * u[j, j2]
                for h in range(2):
                    blk[h] = blk[h] - m * rows[j][h]
            for h in range(2):
                s_ref[SUB * r:SUB * r + SUB, h * NB:(h + 1) * NB] = blk[h]


PB = 256
NP = N // PB


def ds(i, n):
    return pl.ds(pl.multiple_of(i * n, n), n)


def loop(lo, hi, body):
    def step(i, carry):
        body(i)
        return carry
    lax.fori_loop(lo, hi, step, 0)


def tri_iota():
    r = lax.broadcasted_iota(jnp.int32, (NB, NB), 0)
    c = lax.broadcasted_iota(jnp.int32, (NB, NB), 1)
    return r, c


def sweep_body(w_ref, q_ref, s_ref, inv_ref):
    r, c = tri_iota()

    def panel(p):
        def half(h):
            k = 2 * p + h
            rows = ds(k, NB)
            s_ref[:, :NB] = w_ref[rows, rows]
            s_ref[:, NB:] = jnp.where(r == c, 1.0, 0.0).astype(jnp.float32)
            factor_diag(s_ref)
            w_ref[rows, rows] = jnp.where(c >= r, s_ref[:, :NB], 0.0)
            li = s_ref[:, NB:]
            inv_ref[pl.ds(pl.multiple_of(h * NB, NB), NB), pl.ds(pl.multiple_of(h * NB, NB), NB)] = li
            loop(k + 1, N // NB, lambda j: w_ref.__setitem__((rows, ds(j, NB)), mm(li, w_ref[rows, ds(j, NB)])))

            @pl.when(h == 0)
            def _():
                nxt = ds(k + 1, NB)
                lhs = w_ref[rows, nxt]
                def upd(j):
                    w_ref[nxt, ds(j, NB)] = w_ref[nxt, ds(j, NB)] - mm_tn(lhs, w_ref[rows, ds(j, NB)])
                loop(k + 1, N // NB, upd)

        loop(0, 2, half)
        pr = ds(p, PB)
        i0 = inv_ref[:NB, :NB]
        i1 = inv_ref[NB:, NB:]
        u01 = w_ref[ds(2 * p, NB), ds(2 * p + 1, NB)]
        inv_ref[NB:, :NB] = -mm(i1, mm_tn(u01, i0))
        inv_ref[:NB, NB:] = jnp.zeros((NB, NB), jnp.float32)

        def trail(i):
            def cols(j):
                w_ref[ds(i, PB), ds(j, PB)] = w_ref[ds(i, PB), ds(j, PB)] - mm_tn(w_ref[pr, ds(i, PB)], w_ref[pr, ds(j, PB)])
            loop(i, NP, cols)
        loop(p + 1, NP, trail)

        def chunk(m):
            rr = ds(m, PB)
            def prev(t):
                q_ref[rr, pr] = q_ref[rr, pr] - mm(q_ref[rr, ds(t, PB)], w_ref[ds(t, PB), pr])
            loop(0, p, prev)
            q_ref[rr, pr] = mm_nt(q_ref[rr, pr], inv_ref[...])
        loop(0, N // PB, chunk)

    loop(0, NP, panel)

    def zero(k):
        def zz(j):
            w_ref[ds(k, NB), ds(j, NB)] = jnp.zeros((NB, NB), jnp.float32)
        loop(0, k, zz)
    loop(1, N // NB, zero)


VM = pl.BlockSpec(memory_space=pltpu.VMEM)
MESH = pl.DeviceIdType.MESH
TILE = 8
BT = NB // TILE
NBLK = N // NB
HALF = NBLK * (NBLK + 1) // 4 * BT
COL = HALF // 3
QA = COL // 4
QB = QA // 4
AXES = ((0, 1, 2), (1, 2, 0), (2, 0, 1))
STRIDE = (1, 4, 16)
PANELS = (0, 3, 1, 2)


def block_slots():
    slots = {}
    for p in PANELS:
        for i in (2 * p, 2 * p + 1):
            for j in range(i, NBLK):
                slots[i, j] = len(slots)
    return slots


SLOT = block_slots()


def gram_reduce_kernel(a_ref, out_ref, snd, mine, rcv0, rcva, rcvb, rcvc, s_snd, s_rcv):
    core = lax.axis_index("outer")
    row = lax.axis_index("rows")
    pos = (lax.rem(row, 4), lax.rem(row // 4, 4), row // 16)
    partner = (0, 1 - core, row)

    def along(axis, d):
        there = lax.rem(pos[axis] + d, 4)
        return there, (0, core, row + (there - pos[axis]) * STRIDE[axis])

    barrier = pltpu.get_barrier_semaphore()
    peers = [partner] + [along(axis, d)[1] for axis in range(3) for d in (1, 2, 3)]
    for peer in peers:
        pl.semaphore_signal(barrier, inc=1, device_id=peer, device_id_type=MESH)

    count = [0]

    def copy(src, dst, peer):
        k = count[0]
        count[0] += 1
        return pltpu.make_async_remote_copy(src_ref=src, dst_ref=dst, send_sem=s_snd.at[k], recv_sem=s_rcv.at[k], device_id=peer, device_id_type=MESH)

    def products(dst, panels):
        base = SLOT[2 * panels[0], 2 * panels[0]]
        for p in panels:
            for q in range(p, NP):
                g = mm_tn(a_ref[:, p * PB:(p + 1) * PB], a_ref[:, q * PB:(q + 1) * PB])
                for i in (0, 1):
                    for j in (0, 1):
                        if 2 * p + i <= 2 * q + j:
                            k = (SLOT[2 * p + i, 2 * q + j] - base) * BT
                            dst[k:k + BT] = g[i * NB:(i + 1) * NB, j * NB:(j + 1) * NB].reshape(BT, TILE, NB)

    def half_products(dst, own):
        @pl.when(core == (0 if own else 1))
        def _():
            products(dst, PANELS[:2])

        @pl.when(core == (1 if own else 0))
        def _():
            products(dst, PANELS[2:])

    half_products(snd, False)
    pl.semaphore_wait(barrier, len(peers))
    swap = copy(snd, rcv0, partner)
    swap.start()
    half_products(mine, True)
    swap.wait()
    mine[...] = mine[...] + rcv0[...]

    first = []
    for c in range(3):
        ax = AXES[c][0]
        for d in (1, 2, 3):
            there, peer = along(ax, d)
            cp = copy(mine.at[pl.ds(COL * c + QA * there, QA)], rcva.at[c, d - 1], peer)
            cp.start()
            first.append(cp)
    second = []
    for c in range(3):
        for cp in first[3 * c:3 * c + 3]:
            cp.wait_recv()
        off = COL * c + QA * pos[AXES[c][0]]
        mine[pl.ds(off, QA)] = (mine[pl.ds(off, QA)] + rcva[c, 0]) + (rcva[c, 1] + rcva[c, 2])
        for d in (1, 2, 3):
            there, peer = along(AXES[c][1], d)
            cp = copy(mine.at[pl.ds(off + QB * there, QB)], rcvb.at[c, d - 1], peer)
            cp.start()
            second.append(cp)
    third = []
    for c in range(3):
        for cp in second[3 * c:3 * c + 3]:
            cp.wait_recv()
        off = COL * c + QA * pos[AXES[c][0]] + QB * pos[AXES[c][1]]
        here = pos[AXES[c][2]]
        rcvc[c, here] = (mine[pl.ds(off, QB)] + rcvb[c, 0]) + (rcvb[c, 1] + rcvb[c, 2])
        for d in (1, 2, 3):
            _, peer = along(AXES[c][2], d)
            cp = copy(rcvc.at[c, here], rcvc.at[c, here], peer)
            cp.start()
            third.append(cp)
    fourth = []
    for c in range(3):
        for cp in third[3 * c:3 * c + 3]:
            cp.wait()
        off = core * HALF + COL * c + QA * pos[AXES[c][0]] + QB * pos[AXES[c][1]]
        out_ref[pl.ds(off, QB)] = ((rcvc[c, 0] + rcvc[c, 1]) + rcvc[c, 2]) + rcvc[c, 3]
        for d in (1, 2, 3):
            _, peer = along(AXES[c][1], d)
            cp = copy(out_ref.at[pl.ds(off, QB)], out_ref.at[pl.ds(off, QB)], peer)
            cp.start()
            fourth.append(cp)
    fifth = []
    last = []
    for c in range(3):
        for cp in fourth[3 * c:3 * c + 3]:
            cp.wait_recv()
        off = core * HALF + COL * c + QA * pos[AXES[c][0]]
        for d in (1, 2, 3):
            _, peer = along(AXES[c][0], d)
            cp = copy(out_ref.at[pl.ds(off, QA)], out_ref.at[pl.ds(off, QA)], peer)
            cp.start()
            fifth.append(cp)
        cp = copy(out_ref.at[pl.ds(off, QA)], out_ref.at[pl.ds(off, QA)], partner)
        cp.start()
        last.append(cp)
    for c in range(3):
        for d in (1, 2, 3):
            cp = fifth[3 * c + d - 1]
            cp.wait_recv()
            off = core * HALF + COL * c + QA * lax.rem(pos[AXES[c][0]] + 4 - d, 4)
            fw = copy(out_ref.at[pl.ds(off, QA)], out_ref.at[pl.ds(off, QA)], partner)
            fw.start()
            last.append(fw)
    for cp in first + second + fourth + fifth:
        cp.wait_send()
    for cp in last:
        cp.wait()
    assert count[0] == NCOPY


NCOPY = 1 + 9 * 5 + 12


def gram_reduce(a, collective_id=0):
    f32 = jnp.float32
    return pl.pallas_call(
        gram_reduce_kernel,
        out_shape=jax.ShapeDtypeStruct((2 * HALF, TILE, NB), f32),
        in_specs=[VM], out_specs=VM,
        scratch_shapes=[
            pltpu.VMEM((HALF, TILE, NB), f32), pltpu.VMEM((HALF, TILE, NB), f32), pltpu.VMEM((HALF, TILE, NB), f32),
            pltpu.VMEM((3, 3, QA, TILE, NB), f32), pltpu.VMEM((3, 3, QB, TILE, NB), f32), pltpu.VMEM((3, 4, QB, TILE, NB), f32),
            pltpu.SemaphoreType.DMA((NCOPY,)), pltpu.SemaphoreType.DMA((NCOPY,))],
        compiler_params=pltpu.CompilerParams(vmem_limit_bytes=60 * 1024 * 1024, collective_id=collective_id, has_side_effects=True))(a)


def unpack(g_ref, u_ref):
    for (i, j), s in SLOT.items():
        u_ref[i * NB:(i + 1) * NB, j * NB:(j + 1) * NB] = g_ref[s * BT:(s + 1) * BT].reshape(NB, NB)


def first_kernel(g_ref, b_ref, u_ref, q_ref, s_ref, inv_ref):
    unpack(g_ref, u_ref)
    q_ref[...] = b_ref[...]
    sweep_body(u_ref, q_ref, s_ref, inv_ref)


def second_kernel(g_ref, b_ref, u1_ref, r_ref, q_ref, u_ref, s_ref, inv_ref):
    unpack(g_ref, u_ref)
    q_ref[...] = b_ref[...]
    sweep_body(u_ref, q_ref, s_ref, inv_ref)
    r_ref[...] = jnp.zeros((N, N), jnp.float32)

    def ri(i):
        def rj(j):
            def rk(k):
                r_ref[ds(i, PB), ds(j, PB)] = r_ref[ds(i, PB), ds(j, PB)] + mm(u_ref[ds(i, PB), ds(k, PB)], u1_ref[ds(k, PB), ds(j, PB)])
            loop(i, j + 1, rk)
        loop(i, NP, rj)
    loop(0, NP, ri)


SQ = jax.ShapeDtypeStruct((N, N), jnp.float32)
PARAMS = pltpu.CompilerParams(vmem_limit_bytes=60 * 1024 * 1024)
WORK = [pltpu.VMEM((NB, 2 * NB), jnp.float32), pltpu.VMEM((PB, PB), jnp.float32)]


def first_sweep(g, a):
    return pl.pallas_call(first_kernel, out_shape=[SQ, SQ], in_specs=[VM] * 2, out_specs=[VM] * 2, scratch_shapes=WORK, compiler_params=PARAMS)(g, a)


def second_sweep(g, q, u1):
    return pl.pallas_call(second_kernel, out_shape=[SQ, SQ], in_specs=[VM] * 3, out_specs=[VM] * 2, scratch_shapes=[pltpu.VMEM((N, N), jnp.float32)] + WORK, compiler_params=PARAMS)(g, q, u1)


def solution(mesh):
    row_spec = P(("batch", "outer", "rows"), None)

    def group_qr(a_block):
        u1, q1 = first_sweep(gram_reduce(a_block, 0), a_block)
        r_block, q_block = second_sweep(gram_reduce(q1, 1), q1, u1)
        return q_block, r_block

    return jax.shard_map(group_qr, mesh=mesh, in_specs=(row_spec,), out_specs=(row_spec, P("batch", None)), check_vma=False)
```

```python
import functools

import jax
import jax.numpy as jnp
from jax import lax
from jax.experimental import pallas as pl
from jax.experimental.pallas import tpu as pltpu
from jax.sharding import PartitionSpec as P

HI = lax.Precision.HIGHEST
N = 1024
NB = 128
SUB = 8


def mm(a, b):
    return lax.dot_general(a, b, (((1,), (0,)), ((), ())), precision=HI, preferred_element_type=jnp.float32)


def mm_tn(a, b):
    return lax.dot_general(a, b, (((0,), (0,)), ((), ())), precision=HI, preferred_element_type=jnp.float32)


def mm_nt(a, b):
    return lax.dot_general(a, b, (((1,), (1,)), ((), ())), precision=HI, preferred_element_type=jnp.float32)


def lane(v, c):
    return jnp.broadcast_to(v[:, c:c + 1], (SUB, NB))


PB = 256
NP = N // PB


def ds(i, n):
    return pl.ds(pl.multiple_of(i * n, n), n)


def loop(lo, hi, body):
    def step(i, carry):
        body(i)
        return carry
    lax.fori_loop(lo, hi, step, 0)


def factor_diag(s_ref, tasks=()):
    groups = NB // SUB
    tasks = list(tasks)
    for g in range(groups):
        base = SUB * g
        t = []
        for i in range(SUB):
            t.append([jnp.broadcast_to(s_ref[base + i:base + i + 1, h * NB:(h + 1) * NB], (SUB, NB)) for h in range(2)])
        a = {}
        for i in range(SUB):
            for j in range(i, SUB):
                a[i, j] = lane(t[i][0], base + j)
        inv = []
        u = {}
        rows = []
        for j in range(SUB):
            rs = lax.rsqrt(a[j, j])
            inv.append(rs)
            for i in range(j + 1, SUB):
                u[j, i] = a[j, i] * rs
            for i in range(j + 1, SUB):
                for i2 in range(i, SUB):
                    a[i, i2] = a[i, i2] - u[j, i] * u[j, i2]
            row = [t[j][h] * rs for h in range(2)]
            rows.append(row)
            for i in range(j + 1, SUB):
                for h in range(2):
                    t[i][h] = t[i][h] - u[j, i] * row[h]
        for j in range(SUB):
            for h in range(2):
                s_ref[base + j:base + j + 1, h * NB:(h + 1) * NB] = rows[j][h][0:1, :]
        for r in range(g + 1, groups):
            blk = [s_ref[SUB * r:SUB * r + SUB, h * NB:(h + 1) * NB] for h in range(2)]
            v = [lane(blk[0], base + j) for j in range(SUB)]
            for j in range(SUB):
                m = v[j] * inv[j]
                for j2 in range(j + 1, SUB):
                    v[j2] = v[j2] - m * u[j, j2]
                for h in range(2):
                    blk[h] = blk[h] - m * rows[j][h]
            for h in range(2):
                s_ref[SUB * r:SUB * r + SUB, h * NB:(h + 1) * NB] = blk[h]
        if g % 2 == 1 and tasks:
            tasks.pop(0)()
    for task in tasks:
        task()


def sweep_body(w_ref, q_ref, s_ref, inv_ref, prev_ref):
    r = lax.broadcasted_iota(jnp.int32, (NB, NB), 0)
    c = lax.broadcasted_iota(jnp.int32, (NB, NB), 1)

    def diag(k, h, tasks=()):
        rows = ds(k, NB)
        s_ref[:, :NB] = w_ref[rows, rows]
        s_ref[:, NB:] = jnp.where(r == c, 1.0, 0.0).astype(jnp.float32)
        factor_diag(s_ref, tasks)
        w_ref[rows, rows] = jnp.where(c >= r, s_ref[:, :NB], 0.0)
        inv_ref[ds(h, NB), ds(h, NB)] = s_ref[:, NB:]

    def after_first(p):
        top, nxt = ds(2 * p, NB), ds(2 * p + 1, NB)
        u01 = mm(inv_ref[:NB, :NB], w_ref[top, nxt])
        w_ref[top, nxt] = u01
        w_ref[nxt, nxt] = w_ref[nxt, nxt] - mm_tn(u01, u01)
        w_ref[nxt, top] = jnp.zeros((NB, NB), jnp.float32)

    def after_second(p):
        pr = ds(p, PB)
        i0 = inv_ref[:NB, :NB]
        i1 = inv_ref[NB:, NB:]
        inv_ref[NB:, :NB] = -mm(i1, mm_tn(w_ref[ds(2 * p, NB), ds(2 * p + 1, NB)], i0))
        inv_ref[:NB, NB:] = jnp.zeros((NB, NB), jnp.float32)
        prev_ref[...] = inv_ref[...]

        def panel_row(j):
            w_ref[pr, ds(j, PB)] = mm(inv_ref[...], w_ref[pr, ds(j, PB)])
            w_ref[ds(j, PB), pr] = jnp.zeros((PB, PB), jnp.float32)
        loop(p + 1, NP, panel_row)

        def trail(i):
            def cols(j):
                w_ref[ds(i, PB), ds(j, PB)] = w_ref[ds(i, PB), ds(j, PB)] - mm_tn(w_ref[pr, ds(i, PB)], w_ref[pr, ds(j, PB)])
            loop(i, NP, cols)
        loop(p + 1, NP, trail)

    def solve(m, q):
        q_ref[ds(m, PB), ds(q, PB)] = mm_nt(q_ref[ds(m, PB), ds(q, PB)], prev_ref[...])

    def update(m, s, d):
        q_ref[ds(m, PB), ds(d, PB)] = q_ref[ds(m, PB), ds(d, PB)] - mm(q_ref[ds(m, PB), ds(s, PB)], w_ref[ds(s, PB), ds(d, PB)])

    def first_panel(h):
        diag(h, h)
        @pl.when(h == 0)
        def _():
            after_first(0)
    loop(0, 2, first_panel)
    after_second(0)

    def panel(p):
        q = p - 1
        s3 = jnp.where(p == 3, 1, 0)
        d3 = jnp.where(p == 1, 2, 3)
        diag(2 * p, 0, [functools.partial(solve, m, q) for m in range(4)] + [functools.partial(update, m, s3, d3) for m in range(2)])
        after_first(p)
        diag(2 * p + 1, 1, [functools.partial(update, m, q, p) for m in range(4)] + [functools.partial(update, m, s3, d3) for m in range(2, 4)])
        after_second(p)
    loop(1, NP, panel)
    loop(0, NP, lambda m: solve(m, NP - 1))


VM = pl.BlockSpec(memory_space=pltpu.VMEM)
GRAM_VMEM = 18 * 1024 * 1024
SWEEP_VMEM = 30 * 1024 * 1024
MESH = pl.DeviceIdType.MESH
TILE = 8
BT = NB // TILE
NBLK = N // NB
HALF = NBLK * (NBLK + 1) // 4 * BT
COL = HALF // 3
QA = COL // 4
QB = QA // 4
AXES = ((0, 1, 2), (1, 2, 0), (2, 0, 1))
STRIDE = (1, 4, 16)
PANELS = (0, 3, 1, 2)


def block_slots():
    slots = {}
    for p in PANELS:
        for i in (2 * p, 2 * p + 1):
            for j in range(i, NBLK):
                slots[i, j] = len(slots)
    return slots


SLOT = block_slots()


def gram_reduce_kernel(a_ref, out_ref, snd, mine, rcv0, rcva, rcvb, rcvc, s_snd, s_rcv):
    core = lax.axis_index("outer")
    row = lax.axis_index("rows")
    pos = (lax.rem(row, 4), lax.rem(row // 4, 4), row // 16)
    partner = (0, 1 - core, row)

    def along(axis, d):
        there = lax.rem(pos[axis] + d, 4)
        return there, (0, core, row + (there - pos[axis]) * STRIDE[axis])

    barrier = pltpu.get_barrier_semaphore()
    peers = [partner] + [along(axis, d)[1] for axis in range(3) for d in (1, 2, 3)]
    for peer in peers:
        pl.semaphore_signal(barrier, inc=1, device_id=peer, device_id_type=MESH)

    count = [0]

    def copy(src, dst, peer):
        k = count[0]
        count[0] += 1
        return pltpu.make_async_remote_copy(src_ref=src, dst_ref=dst, send_sem=s_snd.at[k], recv_sem=s_rcv.at[k], device_id=peer, device_id_type=MESH)

    def products(dst, s):
        def block(t):
            part = (1 - s) * (t // 4) + s * (t // 3)
            p = (1 - s) * 3 * part + s * (1 + part)
            q = (1 - s) * (t - part) + s * (t + 1 - 2 * part)
            first = (15 - 4 * s) * part
            second = first + N // NB - 2 * p - 1
            g = mm_tn(a_ref[:, ds(p, PB)], a_ref[:, ds(q, PB)])
            for i, j in ((1, 0), (0, 0), (0, 1), (1, 1)):
                k = ((first, second)[i] + 2 * (q - p) + j) * BT
                dst[pl.ds(k, BT)] = g[i * NB:(i + 1) * NB, j * NB:(j + 1) * NB].reshape(BT, TILE, NB)
        loop(0, 5, block)

    products(snd, 1 - core)
    pl.semaphore_wait(barrier, len(peers))
    swap = copy(snd, rcv0, partner)
    swap.start()
    products(mine, core)
    swap.wait()
    mine[...] = mine[...] + rcv0[...]

    first = []
    for c in range(3):
        ax = AXES[c][0]
        for d in (1, 2, 3):
            there, peer = along(ax, d)
            cp = copy(mine.at[pl.ds(COL * c + QA * there, QA)], rcva.at[c, d - 1], peer)
            cp.start()
            first.append(cp)
    second = []
    for c in range(3):
        for cp in first[3 * c:3 * c + 3]:
            cp.wait_recv()
        off = COL * c + QA * pos[AXES[c][0]]
        mine[pl.ds(off, QA)] = (mine[pl.ds(off, QA)] + rcva[c, 0]) + (rcva[c, 1] + rcva[c, 2])
        for d in (1, 2, 3):
            there, peer = along(AXES[c][1], d)
            cp = copy(mine.at[pl.ds(off + QB * there, QB)], rcvb.at[c, d - 1], peer)
            cp.start()
            second.append(cp)
    third = []
    for c in range(3):
        for cp in second[3 * c:3 * c + 3]:
            cp.wait_recv()
        off = COL * c + QA * pos[AXES[c][0]] + QB * pos[AXES[c][1]]
        here = pos[AXES[c][2]]
        rcvc[c, here] = (mine[pl.ds(off, QB)] + rcvb[c, 0]) + (rcvb[c, 1] + rcvb[c, 2])
        for d in (1, 2, 3):
            _, peer = along(AXES[c][2], d)
            cp = copy(rcvc.at[c, here], rcvc.at[c, here], peer)
            cp.start()
            third.append(cp)
    fourth = []
    for c in range(3):
        for cp in third[3 * c:3 * c + 3]:
            cp.wait()
        off = core * HALF + COL * c + QA * pos[AXES[c][0]] + QB * pos[AXES[c][1]]
        out_ref[pl.ds(off, QB)] = ((rcvc[c, 0] + rcvc[c, 1]) + rcvc[c, 2]) + rcvc[c, 3]
        for d in (1, 2, 3):
            _, peer = along(AXES[c][1], d)
            cp = copy(out_ref.at[pl.ds(off, QB)], out_ref.at[pl.ds(off, QB)], peer)
            cp.start()
            fourth.append(cp)
    fifth = []
    last = []
    for c in range(3):
        for cp in fourth[3 * c:3 * c + 3]:
            cp.wait_recv()
        off = core * HALF + COL * c + QA * pos[AXES[c][0]]
        for d in (1, 2, 3):
            _, peer = along(AXES[c][0], d)
            cp = copy(out_ref.at[pl.ds(off, QA)], out_ref.at[pl.ds(off, QA)], peer)
            cp.start()
            fifth.append(cp)
        cp = copy(out_ref.at[pl.ds(off, QA)], out_ref.at[pl.ds(off, QA)], partner)
        cp.start()
        last.append(cp)
    for c in range(3):
        for d in (1, 2, 3):
            cp = fifth[3 * c + d - 1]
            cp.wait_recv()
            off = core * HALF + COL * c + QA * lax.rem(pos[AXES[c][0]] + 4 - d, 4)
            fw = copy(out_ref.at[pl.ds(off, QA)], out_ref.at[pl.ds(off, QA)], partner)
            fw.start()
            last.append(fw)
    for cp in first + second + fourth + fifth:
        cp.wait_send()
    for cp in last:
        cp.wait()
    assert count[0] == NCOPY


NCOPY = 1 + 9 * 5 + 12


def gram_reduce(a, collective_id=0):
    f32 = jnp.float32
    return pl.pallas_call(
        gram_reduce_kernel,
        out_shape=jax.ShapeDtypeStruct((2 * HALF, TILE, NB), f32),
        in_specs=[VM], out_specs=VM,
        scratch_shapes=[
            pltpu.VMEM((HALF, TILE, NB), f32), pltpu.VMEM((HALF, TILE, NB), f32), pltpu.VMEM((HALF, TILE, NB), f32),
            pltpu.VMEM((3, 3, QA, TILE, NB), f32), pltpu.VMEM((3, 3, QB, TILE, NB), f32), pltpu.VMEM((3, 4, QB, TILE, NB), f32),
            pltpu.SemaphoreType.DMA((NCOPY,)), pltpu.SemaphoreType.DMA((NCOPY,))],
        compiler_params=pltpu.CompilerParams(vmem_limit_bytes=GRAM_VMEM, collective_id=collective_id, has_side_effects=True))(a)


def unpack(g_ref, u_ref):
    for (i, j), s in SLOT.items():
        u_ref[i * NB:(i + 1) * NB, j * NB:(j + 1) * NB] = g_ref[s * BT:(s + 1) * BT].reshape(NB, NB)


def first_kernel(g_ref, b_ref, u_ref, q_ref, s_ref, inv_ref, prev_ref):
    unpack(g_ref, u_ref)
    q_ref[...] = b_ref[...]
    sweep_body(u_ref, q_ref, s_ref, inv_ref, prev_ref)


def second_kernel(g_ref, b_ref, u1_ref, r_ref, q_ref, u_ref, s_ref, inv_ref, prev_ref):
    unpack(g_ref, u_ref)
    q_ref[...] = b_ref[...]
    sweep_body(u_ref, q_ref, s_ref, inv_ref, prev_ref)
    r_ref[...] = jnp.zeros((N, N), jnp.float32)

    def ri(i):
        def rj(j):
            def rk(k):
                r_ref[ds(i, PB), ds(j, PB)] = r_ref[ds(i, PB), ds(j, PB)] + mm(u_ref[ds(i, PB), ds(k, PB)], u1_ref[ds(k, PB), ds(j, PB)])
            loop(i, j + 1, rk)
        loop(i, NP, rj)
    loop(0, NP, ri)


SQ = jax.ShapeDtypeStruct((N, N), jnp.float32)
WORK = [pltpu.VMEM((NB, 2 * NB), jnp.float32), pltpu.VMEM((PB, PB), jnp.float32), pltpu.VMEM((PB, PB), jnp.float32)]


def first_sweep(g, a):
    return pl.pallas_call(first_kernel, out_shape=[SQ, SQ], in_specs=[VM] * 2, out_specs=[VM] * 2, scratch_shapes=WORK, compiler_params=pltpu.CompilerParams(vmem_limit_bytes=SWEEP_VMEM))(g, a)


def second_sweep(g, q, u1):
    return pl.pallas_call(second_kernel, out_shape=[SQ, SQ], in_specs=[VM] * 3, out_specs=[VM] * 2, scratch_shapes=[pltpu.VMEM((N, N), jnp.float32)] + WORK, compiler_params=pltpu.CompilerParams(vmem_limit_bytes=SWEEP_VMEM))(g, q, u1)


def solution(mesh):
    row_spec = P(("batch", "outer", "rows"), None)

    def group_qr(a_block):
        u1, q1 = first_sweep(gram_reduce(a_block, 0), a_block)
        r_block, q_block = second_sweep(gram_reduce(q1, 1), q1, u1)
        return q_block, r_block

    return jax.shard_map(group_qr, mesh=mesh, in_specs=(row_spec,), out_specs=(row_spec, P("batch", None)), check_vma=False)
```

```python
import functools

import jax
import jax.numpy as jnp
from jax import lax
from jax.experimental import pallas as pl
from jax.experimental.pallas import tpu as pltpu
from jax.sharding import PartitionSpec as P

HI = lax.Precision.HIGHEST
N = 1024
NB = 128
SUB = 8


def mm(a, b):
    return lax.dot_general(a, b, (((1,), (0,)), ((), ())), precision=HI, preferred_element_type=jnp.float32)


def mm_tn(a, b):
    return lax.dot_general(a, b, (((0,), (0,)), ((), ())), precision=HI, preferred_element_type=jnp.float32)


def mm_nt(a, b):
    return lax.dot_general(a, b, (((1,), (1,)), ((), ())), precision=HI, preferred_element_type=jnp.float32)


def lane(v, c):
    return jnp.broadcast_to(v[:, c:c + 1], (SUB, NB))


PB = 256
NP = N // PB


def ds(i, n):
    return pl.ds(pl.multiple_of(i * n, n), n)


def loop(lo, hi, body):
    def step(i, carry):
        body(i)
        return carry
    lax.fori_loop(lo, hi, step, 0)


RG = 15


def factor_diag(s_ref, tasks=()):
    groups = NB // SUB
    tasks = list(tasks)
    for g in range(groups):
        base = SUB * g
        left = jnp.stack([jnp.broadcast_to(s_ref[base + i:base + i + 1, :NB], (SUB, NB)) for i in range(SUB)])
        right = jnp.stack([jnp.broadcast_to(s_ref[base + i:base + i + 1, NB:], (SUB, NB)) for i in range(SUB)])
        a = [jnp.stack([lane(left[j], base + i) for i in range(j, SUB)]) for j in range(SUB)]
        inv, u, rows = [], [], []
        for j in range(SUB):
            rs = lax.rsqrt(a[j][0])
            inv.append(rs)
            rl, rr = left[0] * rs, right[0] * rs
            rows.append((rl, rr))
            s_ref[base + j:base + j + 1, :NB] = rl[0:1]
            s_ref[base + j:base + j + 1, NB:] = rr[0:1]
            if j + 1 < SUB:
                uj = a[j][1:] * rs
                u.append(uj)
                for i in range(j + 1, SUB):
                    a[i] = a[i] - uj[i - j - 1:] * uj[i - j - 1]
                left = left[1:] - uj * rl
                right = right[1:] - uj * rr
        for lo in range(g + 1, groups, RG):
            hi = min(lo + RG, groups)
            n = hi - lo
            at = slice(SUB * lo, SUB * hi)
            bl = s_ref[at, :NB].reshape(n, SUB, NB)
            br = s_ref[at, NB:].reshape(n, SUB, NB)
            v = [jnp.broadcast_to(bl[:, :, base + j:base + j + 1], (n, SUB, NB)) for j in range(SUB)]
            for j in range(SUB):
                m = v[j] * inv[j]
                for j2 in range(j + 1, SUB):
                    v[j2] = v[j2] - m * u[j][j2 - j - 1]
                bl = bl - m * rows[j][0]
                br = br - m * rows[j][1]
            s_ref[at, :NB] = bl.reshape(n * SUB, NB)
            s_ref[at, NB:] = br.reshape(n * SUB, NB)
        if g % 2 == 1 and tasks:
            tasks.pop(0)()
    for task in tasks:
        task()


def sweep_body(w_ref, q_ref, s_ref, inv_ref, prev_ref):
    r = lax.broadcasted_iota(jnp.int32, (NB, NB), 0)
    c = lax.broadcasted_iota(jnp.int32, (NB, NB), 1)

    def diag(k, h, tasks=()):
        rows = ds(k, NB)
        s_ref[:, :NB] = w_ref[rows, rows]
        s_ref[:, NB:] = jnp.where(r == c, 1.0, 0.0).astype(jnp.float32)
        factor_diag(s_ref, tasks)
        w_ref[rows, rows] = jnp.where(c >= r, s_ref[:, :NB], 0.0)
        inv_ref[ds(h, NB), ds(h, NB)] = s_ref[:, NB:]

    def after_first(p):
        top, nxt = ds(2 * p, NB), ds(2 * p + 1, NB)
        u01 = mm(inv_ref[:NB, :NB], w_ref[top, nxt])
        w_ref[top, nxt] = u01
        w_ref[nxt, nxt] = w_ref[nxt, nxt] - mm_tn(u01, u01)
        w_ref[nxt, top] = jnp.zeros((NB, NB), jnp.float32)

    def after_second(p):
        pr = ds(p, PB)
        i0 = inv_ref[:NB, :NB]
        i1 = inv_ref[NB:, NB:]
        inv_ref[NB:, :NB] = -mm(i1, mm_tn(w_ref[ds(2 * p, NB), ds(2 * p + 1, NB)], i0))
        inv_ref[:NB, NB:] = jnp.zeros((NB, NB), jnp.float32)
        prev_ref[...] = inv_ref[...]

        def panel_row(j):
            w_ref[pr, ds(j, PB)] = mm(inv_ref[...], w_ref[pr, ds(j, PB)])
            w_ref[ds(j, PB), pr] = jnp.zeros((PB, PB), jnp.float32)
        loop(p + 1, NP, panel_row)

        def trail(i):
            def cols(j):
                w_ref[ds(i, PB), ds(j, PB)] = w_ref[ds(i, PB), ds(j, PB)] - mm_tn(w_ref[pr, ds(i, PB)], w_ref[pr, ds(j, PB)])
            loop(i, NP, cols)
        loop(p + 1, NP, trail)

    def solve(m, q):
        q_ref[ds(m, PB), ds(q, PB)] = mm_nt(q_ref[ds(m, PB), ds(q, PB)], prev_ref[...])

    def update(m, s, d):
        q_ref[ds(m, PB), ds(d, PB)] = q_ref[ds(m, PB), ds(d, PB)] - mm(q_ref[ds(m, PB), ds(s, PB)], w_ref[ds(s, PB), ds(d, PB)])

    def first_panel(h):
        diag(h, h)
        @pl.when(h == 0)
        def _():
            after_first(0)
    loop(0, 2, first_panel)
    after_second(0)

    def panel(p):
        q = p - 1
        s3 = jnp.where(p == 3, 1, 0)
        d3 = jnp.where(p == 1, 2, 3)
        diag(2 * p, 0, [functools.partial(solve, m, q) for m in range(4)] + [functools.partial(update, m, s3, d3) for m in range(2)])
        after_first(p)
        diag(2 * p + 1, 1, [functools.partial(update, m, q, p) for m in range(4)] + [functools.partial(update, m, s3, d3) for m in range(2, 4)])
        after_second(p)
    loop(1, NP, panel)
    loop(0, NP, lambda m: solve(m, NP - 1))


VM = pl.BlockSpec(memory_space=pltpu.VMEM)
GRAM_VMEM = 18 * 1024 * 1024
SWEEP_VMEM = 30 * 1024 * 1024
MESH = pl.DeviceIdType.MESH
TILE = 8
BT = NB // TILE
NBLK = N // NB
HALF = NBLK * (NBLK + 1) // 4 * BT
COL = HALF // 3
QA = COL // 4
QB = QA // 4
AXES = ((0, 1, 2), (1, 2, 0), (2, 0, 1))
STRIDE = (1, 4, 16)
PANELS = (0, 3, 1, 2)


def block_slots():
    slots = {}
    for p in PANELS:
        for i in (2 * p, 2 * p + 1):
            for j in range(i, NBLK):
                slots[i, j] = len(slots)
    return slots


SLOT = block_slots()


def gram_reduce_kernel(a_ref, out_ref, snd, mine, rcv0, rcva, rcvb, rcvc, s_snd, s_rcv):
    core = lax.axis_index("outer")
    row = lax.axis_index("rows")
    pos = (lax.rem(row, 4), lax.rem(row // 4, 4), row // 16)
    partner = (0, 1 - core, row)

    def along(axis, d):
        there = lax.rem(pos[axis] + d, 4)
        return there, (0, core, row + (there - pos[axis]) * STRIDE[axis])

    barrier = pltpu.get_barrier_semaphore()
    peers = [partner] + [along(axis, d)[1] for axis in range(3) for d in (1, 2, 3)]
    for peer in peers:
        pl.semaphore_signal(barrier, inc=1, device_id=peer, device_id_type=MESH)

    count = [0]

    def copy(src, dst, peer):
        k = count[0]
        count[0] += 1
        return pltpu.make_async_remote_copy(src_ref=src, dst_ref=dst, send_sem=s_snd.at[k], recv_sem=s_rcv.at[k], device_id=peer, device_id_type=MESH)

    def products(dst, s):
        def block(t):
            part = (1 - s) * (t // 4) + s * (t // 3)
            p = (1 - s) * 3 * part + s * (1 + part)
            q = (1 - s) * (t - part) + s * (t + 1 - 2 * part)
            first = (15 - 4 * s) * part
            second = first + N // NB - 2 * p - 1
            g = mm_tn(a_ref[:, ds(p, PB)], a_ref[:, ds(q, PB)])
            for i, j in ((1, 0), (0, 0), (0, 1), (1, 1)):
                k = ((first, second)[i] + 2 * (q - p) + j) * BT
                dst[pl.ds(k, BT)] = g[i * NB:(i + 1) * NB, j * NB:(j + 1) * NB].reshape(BT, TILE, NB)
        loop(0, 5, block)

    products(snd, 1 - core)
    pl.semaphore_wait(barrier, len(peers))
    swap = copy(snd, rcv0, partner)
    swap.start()
    products(mine, core)
    swap.wait()
    mine[...] = mine[...] + rcv0[...]

    first = []
    for c in range(3):
        ax = AXES[c][0]
        for d in (1, 2, 3):
            there, peer = along(ax, d)
            cp = copy(mine.at[pl.ds(COL * c + QA * there, QA)], rcva.at[c, d - 1], peer)
            cp.start()
            first.append(cp)
    second = []
    for c in range(3):
        for cp in first[3 * c:3 * c + 3]:
            cp.wait_recv()
        off = COL * c + QA * pos[AXES[c][0]]
        mine[pl.ds(off, QA)] = (mine[pl.ds(off, QA)] + rcva[c, 0]) + (rcva[c, 1] + rcva[c, 2])
        for d in (1, 2, 3):
            there, peer = along(AXES[c][1], d)
            cp = copy(mine.at[pl.ds(off + QB * there, QB)], rcvb.at[c, d - 1], peer)
            cp.start()
            second.append(cp)
    third = []
    for c in range(3):
        for cp in second[3 * c:3 * c + 3]:
            cp.wait_recv()
        off = COL * c + QA * pos[AXES[c][0]] + QB * pos[AXES[c][1]]
        here = pos[AXES[c][2]]
        rcvc[c, here] = (mine[pl.ds(off, QB)] + rcvb[c, 0]) + (rcvb[c, 1] + rcvb[c, 2])
        for d in (1, 2, 3):
            _, peer = along(AXES[c][2], d)
            cp = copy(rcvc.at[c, here], rcvc.at[c, here], peer)
            cp.start()
            third.append(cp)
    fourth = []
    for c in range(3):
        for cp in third[3 * c:3 * c + 3]:
            cp.wait()
        off = core * HALF + COL * c + QA * pos[AXES[c][0]] + QB * pos[AXES[c][1]]
        out_ref[pl.ds(off, QB)] = ((rcvc[c, 0] + rcvc[c, 1]) + rcvc[c, 2]) + rcvc[c, 3]
        for d in (1, 2, 3):
            _, peer = along(AXES[c][1], d)
            cp = copy(out_ref.at[pl.ds(off, QB)], out_ref.at[pl.ds(off, QB)], peer)
            cp.start()
            fourth.append(cp)
    fifth = []
    last = []
    for c in range(3):
        for cp in fourth[3 * c:3 * c + 3]:
            cp.wait_recv()
        off = core * HALF + COL * c + QA * pos[AXES[c][0]]
        for d in (1, 2, 3):
            _, peer = along(AXES[c][0], d)
            cp = copy(out_ref.at[pl.ds(off, QA)], out_ref.at[pl.ds(off, QA)], peer)
            cp.start()
            fifth.append(cp)
        cp = copy(out_ref.at[pl.ds(off, QA)], out_ref.at[pl.ds(off, QA)], partner)
        cp.start()
        last.append(cp)
    for c in range(3):
        for d in (1, 2, 3):
            cp = fifth[3 * c + d - 1]
            cp.wait_recv()
            off = core * HALF + COL * c + QA * lax.rem(pos[AXES[c][0]] + 4 - d, 4)
            fw = copy(out_ref.at[pl.ds(off, QA)], out_ref.at[pl.ds(off, QA)], partner)
            fw.start()
            last.append(fw)
    for cp in first + second + fourth + fifth:
        cp.wait_send()
    for cp in last:
        cp.wait()
    assert count[0] == NCOPY


NCOPY = 1 + 9 * 5 + 12


def comm_scratch():
    f32 = jnp.float32
    return [
            pltpu.VMEM((HALF, TILE, NB), f32), pltpu.VMEM((HALF, TILE, NB), f32), pltpu.VMEM((HALF, TILE, NB), f32),
            pltpu.VMEM((3, 3, QA, TILE, NB), f32), pltpu.VMEM((3, 3, QB, TILE, NB), f32), pltpu.VMEM((3, 4, QB, TILE, NB), f32),
            pltpu.SemaphoreType.DMA((NCOPY,)), pltpu.SemaphoreType.DMA((NCOPY,))]


def gram_reduce(a, collective_id=0):
    f32 = jnp.float32
    return pl.pallas_call(
        gram_reduce_kernel,
        out_shape=jax.ShapeDtypeStruct((2 * HALF, TILE, NB), f32),
        in_specs=[VM], out_specs=VM,
        scratch_shapes=comm_scratch(),
        compiler_params=pltpu.CompilerParams(vmem_limit_bytes=GRAM_VMEM, collective_id=collective_id, has_side_effects=True))(a)


def unpack(g_ref, u_ref):
    for (i, j), s in SLOT.items():
        u_ref[i * NB:(i + 1) * NB, j * NB:(j + 1) * NB] = g_ref[s * BT:(s + 1) * BT].reshape(NB, NB)


def tri_iota():
    r = lax.broadcasted_iota(jnp.int32, (NB, NB), 0)
    c = lax.broadcasted_iota(jnp.int32, (NB, NB), 1)
    return r, c


def sweep_one(w_ref, q_ref, s_ref, inv_ref):
    r, c = tri_iota()

    def panel(p):
        def half(h):
            k = 2 * p + h
            rows = ds(k, NB)
            s_ref[:, :NB] = w_ref[rows, rows]
            s_ref[:, NB:] = jnp.where(r == c, 1.0, 0.0).astype(jnp.float32)
            factor_diag(s_ref)
            w_ref[rows, rows] = jnp.where(c >= r, s_ref[:, :NB], 0.0)
            li = s_ref[:, NB:]
            inv_ref[pl.ds(pl.multiple_of(h * NB, NB), NB), pl.ds(pl.multiple_of(h * NB, NB), NB)] = li
            loop(k + 1, N // NB, lambda j: w_ref.__setitem__((rows, ds(j, NB)), mm(li, w_ref[rows, ds(j, NB)])))

            @pl.when(h == 0)
            def _():
                nxt = ds(k + 1, NB)
                lhs = w_ref[rows, nxt]
                def upd(j):
                    w_ref[nxt, ds(j, NB)] = w_ref[nxt, ds(j, NB)] - mm_tn(lhs, w_ref[rows, ds(j, NB)])
                loop(k + 1, N // NB, upd)

        loop(0, 2, half)
        pr = ds(p, PB)
        i0 = inv_ref[:NB, :NB]
        i1 = inv_ref[NB:, NB:]
        u01 = w_ref[ds(2 * p, NB), ds(2 * p + 1, NB)]
        inv_ref[NB:, :NB] = -mm(i1, mm_tn(u01, i0))
        inv_ref[:NB, NB:] = jnp.zeros((NB, NB), jnp.float32)

        def trail(i):
            def cols(j):
                w_ref[ds(i, PB), ds(j, PB)] = w_ref[ds(i, PB), ds(j, PB)] - mm_tn(w_ref[pr, ds(i, PB)], w_ref[pr, ds(j, PB)])
            loop(i, NP, cols)
        loop(p + 1, NP, trail)

        def chunk(m):
            rr = ds(m, PB)
            def prev(t):
                q_ref[rr, pr] = q_ref[rr, pr] - mm(q_ref[rr, ds(t, PB)], w_ref[ds(t, PB), pr])
            loop(0, p, prev)
            q_ref[rr, pr] = mm_nt(q_ref[rr, pr], inv_ref[...])
        loop(0, N // PB, chunk)

    loop(0, NP, panel)

    def zero(k):
        def zz(j):
            w_ref[ds(k, NB), ds(j, NB)] = jnp.zeros((NB, NB), jnp.float32)
        loop(0, k, zz)
    loop(1, N // NB, zero)


def fused_kernel(g_ref, b_ref, u_ref, q_ref, out_ref, s_ref, inv_ref, prev_ref, *rest):
    unpack(g_ref, u_ref)
    q_ref[...] = b_ref[...]
    sweep_one(u_ref, q_ref, s_ref, inv_ref)
    gram_reduce_kernel(q_ref, out_ref, *rest)


def second_kernel(g_ref, b_ref, u1_ref, r_ref, q_ref, u_ref, s_ref, inv_ref, prev_ref):
    unpack(g_ref, u_ref)
    q_ref[...] = b_ref[...]
    sweep_body(u_ref, q_ref, s_ref, inv_ref, prev_ref)
    r_ref[...] = jnp.zeros((N, N), jnp.float32)

    def ri(i):
        def rj(j):
            def rk(k):
                r_ref[ds(i, PB), ds(j, PB)] = r_ref[ds(i, PB), ds(j, PB)] + mm(u_ref[ds(i, PB), ds(k, PB)], u1_ref[ds(k, PB), ds(j, PB)])
            loop(i, j + 1, rk)
        loop(i, NP, rj)
    loop(0, NP, ri)


SQ = jax.ShapeDtypeStruct((N, N), jnp.float32)
WORK = [pltpu.VMEM((NB, 2 * NB), jnp.float32), pltpu.VMEM((PB, PB), jnp.float32), pltpu.VMEM((PB, PB), jnp.float32)]


def first_sweep(g, a):
    return pl.pallas_call(
        fused_kernel, out_shape=[SQ, SQ, jax.ShapeDtypeStruct((2 * HALF, TILE, NB), jnp.float32)], in_specs=[VM] * 2, out_specs=[VM] * 3, scratch_shapes=WORK + comm_scratch(),
        compiler_params=pltpu.CompilerParams(vmem_limit_bytes=SWEEP_VMEM, collective_id=1, has_side_effects=True))(g, a)


def second_sweep(g, q, u1):
    return pl.pallas_call(second_kernel, out_shape=[SQ, SQ], in_specs=[VM] * 3, out_specs=[VM] * 2, scratch_shapes=[pltpu.VMEM((N, N), jnp.float32)] + WORK, compiler_params=pltpu.CompilerParams(vmem_limit_bytes=SWEEP_VMEM))(g, q, u1)


def solution(mesh):
    row_spec = P(("batch", "outer", "rows"), None)

    def group_qr(a_block):
        u1, q1, g2 = first_sweep(gram_reduce(a_block, 0), a_block)
        r_block, q_block = second_sweep(g2, q1, u1)
        return q_block, r_block

    return jax.shard_map(group_qr, mesh=mesh, in_specs=(row_spec,), out_specs=(row_spec, P("batch", None)), check_vma=False)
```

```python
import functools

import jax
import jax.numpy as jnp
from jax import lax
from jax.experimental import pallas as pl
from jax.experimental.pallas import tpu as pltpu
from jax.sharding import PartitionSpec as P

HI = lax.Precision.HIGHEST
N = 1024
NB = 128
SUB = 8


def mm(a, b):
    return lax.dot_general(a, b, (((1,), (0,)), ((), ())), precision=HI, preferred_element_type=jnp.float32)


def mm_tn(a, b):
    return lax.dot_general(a, b, (((0,), (0,)), ((), ())), precision=HI, preferred_element_type=jnp.float32)


def mm_nt(a, b):
    return lax.dot_general(a, b, (((1,), (1,)), ((), ())), precision=HI, preferred_element_type=jnp.float32)


def lane(v, c):
    return jnp.broadcast_to(v[:, c:c + 1], (SUB, NB))


PB = 256
NP = N // PB


def ds(i, n):
    return pl.ds(pl.multiple_of(i * n, n), n)


def loop(lo, hi, body):
    def step(i, carry):
        body(i)
        return carry
    lax.fori_loop(lo, hi, step, 0)


RG = 3


def factor_diag(s_ref, tasks=()):
    groups = NB // SUB
    tasks = list(tasks)
    for g in range(groups):
        base = SUB * g
        left = jnp.stack([jnp.broadcast_to(s_ref[base + i:base + i + 1, :NB], (SUB, NB)) for i in range(SUB)])
        right = jnp.stack([jnp.broadcast_to(s_ref[base + i:base + i + 1, NB:], (SUB, NB)) for i in range(SUB)])
        a = [jnp.stack([lane(left[j], base + i) for i in range(j, SUB)]) for j in range(SUB)]
        inv, u, rows = [], [], []
        for j in range(SUB):
            rs = lax.rsqrt(a[j][0])
            inv.append(rs)
            rl, rr = left[0] * rs, right[0] * rs
            rows.append((rl, rr))
            s_ref[base + j:base + j + 1, :NB] = rl[0:1]
            s_ref[base + j:base + j + 1, NB:] = rr[0:1]
            if j + 1 < SUB:
                uj = a[j][1:] * rs
                u.append(uj)
                for i in range(j + 1, SUB):
                    a[i] = a[i] - uj[i - j - 1:] * uj[i - j - 1]
                left = left[1:] - uj * rl
                right = right[1:] - uj * rr
        for lo in range(g + 1, groups, RG):
            hi = min(lo + RG, groups)
            n = hi - lo
            at = slice(SUB * lo, SUB * hi)
            bl = s_ref[at, :NB].reshape(n, SUB, NB)
            br = s_ref[at, NB:].reshape(n, SUB, NB)
            v = [jnp.broadcast_to(bl[:, :, base + j:base + j + 1], (n, SUB, NB)) for j in range(SUB)]
            for j in range(SUB):
                m = v[j] * inv[j]
                for j2 in range(j + 1, SUB):
                    v[j2] = v[j2] - m * u[j][j2 - j - 1]
                bl = bl - m * rows[j][0]
                br = br - m * rows[j][1]
            s_ref[at, :NB] = bl.reshape(n * SUB, NB)
            s_ref[at, NB:] = br.reshape(n * SUB, NB)
        if g % 2 == 1 and tasks:
            tasks.pop(0)()
    for task in tasks:
        task()


VM = pl.BlockSpec(memory_space=pltpu.VMEM)
GRAM_VMEM = 18 * 1024 * 1024
SWEEP_VMEM = 42 * 1024 * 1024
FINISH_VMEM = 24 * 1024 * 1024
MESH = pl.DeviceIdType.MESH
TILE = 8
BT = NB // TILE
NBLK = N // NB
HALF = NBLK * (NBLK + 1) // 4 * BT
COL = HALF // 3
QA = COL // 4
QB = QA // 4
AXES = ((0, 1, 2), (1, 2, 0), (2, 0, 1))
STRIDE = (1, 4, 16)
PANELS = (0, 3, 1, 2)


def block_slots():
    slots = {}
    for p in PANELS:
        for i in (2 * p, 2 * p + 1):
            for j in range(i, NBLK):
                slots[i, j] = len(slots)
    return slots


SLOT = block_slots()


def gram_reduce_kernel(a_ref, out_ref, snd, mine, rcv0, rcva, rcvb, rcvc, s_snd, s_rcv):
    core = lax.axis_index("outer")
    row = lax.axis_index("rows")
    pos = (lax.rem(row, 4), lax.rem(row // 4, 4), row // 16)
    partner = (0, 1 - core, row)

    def along(axis, d):
        there = lax.rem(pos[axis] + d, 4)
        return there, (0, core, row + (there - pos[axis]) * STRIDE[axis])

    barrier = pltpu.get_barrier_semaphore()
    peers = [partner] + [along(axis, d)[1] for axis in range(3) for d in (1, 2, 3)]
    for peer in peers:
        pl.semaphore_signal(barrier, inc=1, device_id=peer, device_id_type=MESH)

    count = [0]

    def copy(src, dst, peer):
        k = count[0]
        count[0] += 1
        return pltpu.make_async_remote_copy(src_ref=src, dst_ref=dst, send_sem=s_snd.at[k], recv_sem=s_rcv.at[k], device_id=peer, device_id_type=MESH)

    def products(dst, s):
        def block(t):
            part = (1 - s) * (t // 4) + s * (t // 3)
            p = (1 - s) * 3 * part + s * (1 + part)
            q = (1 - s) * (t - part) + s * (t + 1 - 2 * part)
            first = (15 - 4 * s) * part
            second = first + N // NB - 2 * p - 1
            g = mm_tn(a_ref[:, ds(p, PB)], a_ref[:, ds(q, PB)])
            for i, j in ((1, 0), (0, 0), (0, 1), (1, 1)):
                k = ((first, second)[i] + 2 * (q - p) + j) * BT
                dst[pl.ds(k, BT)] = g[i * NB:(i + 1) * NB, j * NB:(j + 1) * NB].reshape(BT, TILE, NB)
        loop(0, 5, block)

    products(snd, 1 - core)
    pl.semaphore_wait(barrier, len(peers))
    swap = copy(snd, rcv0, partner)
    swap.start()
    products(mine, core)
    swap.wait()
    mine[...] = mine[...] + rcv0[...]

    first = []
    for c in range(3):
        ax = AXES[c][0]
        for d in (1, 2, 3):
            there, peer = along(ax, d)
            cp = copy(mine.at[pl.ds(COL * c + QA * there, QA)], rcva.at[c, d - 1], peer)
            cp.start()
            first.append(cp)
    second = []
    for c in range(3):
        for cp in first[3 * c:3 * c + 3]:
            cp.wait_recv()
        off = COL * c + QA * pos[AXES[c][0]]
        mine[pl.ds(off, QA)] = (mine[pl.ds(off, QA)] + rcva[c, 0]) + (rcva[c, 1] + rcva[c, 2])
        for d in (1, 2, 3):
            there, peer = along(AXES[c][1], d)
            cp = copy(mine.at[pl.ds(off + QB * there, QB)], rcvb.at[c, d - 1], peer)
            cp.start()
            second.append(cp)
    third = []
    for c in range(3):
        for cp in second[3 * c:3 * c + 3]:
            cp.wait_recv()
        off = COL * c + QA * pos[AXES[c][0]] + QB * pos[AXES[c][1]]
        here = pos[AXES[c][2]]
        rcvc[c, here] = (mine[pl.ds(off, QB)] + rcvb[c, 0]) + (rcvb[c, 1] + rcvb[c, 2])
        for d in (1, 2, 3):
            _, peer = along(AXES[c][2], d)
            cp = copy(rcvc.at[c, here], rcvc.at[c, here], peer)
            cp.start()
            third.append(cp)
    fourth = []
    for c in range(3):
        for cp in third[3 * c:3 * c + 3]:
            cp.wait()
        off = core * HALF + COL * c + QA * pos[AXES[c][0]] + QB * pos[AXES[c][1]]
        out_ref[pl.ds(off, QB)] = ((rcvc[c, 0] + rcvc[c, 1]) + rcvc[c, 2]) + rcvc[c, 3]
        for d in (1, 2, 3):
            _, peer = along(AXES[c][1], d)
            cp = copy(out_ref.at[pl.ds(off, QB)], out_ref.at[pl.ds(off, QB)], peer)
            cp.start()
            fourth.append(cp)
    fifth = []
    last = []
    for c in range(3):
        for cp in fourth[3 * c:3 * c + 3]:
            cp.wait_recv()
        off = core * HALF + COL * c + QA * pos[AXES[c][0]]
        for d in (1, 2, 3):
            _, peer = along(AXES[c][0], d)
            cp = copy(out_ref.at[pl.ds(off, QA)], out_ref.at[pl.ds(off, QA)], peer)
            cp.start()
            fifth.append(cp)
        cp = copy(out_ref.at[pl.ds(off, QA)], out_ref.at[pl.ds(off, QA)], partner)
        cp.start()
        last.append(cp)
    for c in range(3):
        for d in (1, 2, 3):
            cp = fifth[3 * c + d - 1]
            cp.wait_recv()
            off = core * HALF + COL * c + QA * lax.rem(pos[AXES[c][0]] + 4 - d, 4)
            fw = copy(out_ref.at[pl.ds(off, QA)], out_ref.at[pl.ds(off, QA)], partner)
            fw.start()
            last.append(fw)
    for cp in first + second + fourth + fifth:
        cp.wait_send()
    for cp in last:
        cp.wait()
    assert count[0] == NCOPY


NCOPY = 1 + 9 * 5 + 12


def gram_reduce(a, collective_id=0):
    f32 = jnp.float32
    return pl.pallas_call(
        gram_reduce_kernel,
        out_shape=jax.ShapeDtypeStruct((2 * HALF, TILE, NB), f32),
        in_specs=[VM], out_specs=VM,
        scratch_shapes=[
            pltpu.VMEM((HALF, TILE, NB), f32), pltpu.VMEM((HALF, TILE, NB), f32), pltpu.VMEM((HALF, TILE, NB), f32),
            pltpu.VMEM((3, 3, QA, TILE, NB), f32), pltpu.VMEM((3, 3, QB, TILE, NB), f32), pltpu.VMEM((3, 4, QB, TILE, NB), f32),
            pltpu.SemaphoreType.DMA((NCOPY,)), pltpu.SemaphoreType.DMA((NCOPY,))],
        compiler_params=pltpu.CompilerParams(vmem_limit_bytes=GRAM_VMEM, collective_id=collective_id, has_side_effects=True))(a)


def unpack(g_ref, u_ref):
    for (i, j), s in SLOT.items():
        u_ref[i * NB:(i + 1) * NB, j * NB:(j + 1) * NB] = g_ref[s * BT:(s + 1) * BT].reshape(NB, NB)


SIZES = (96, 192, 192, 288)
COPIES = 1 + 9 * 5 + 12


class PanelSum:
    def __init__(self, n, buf, rcv0, rcva, rcvb, rcvc, out, s_snd, s_rcv, place):
        self.size = SIZES[n]
        self.half = self.size // 2
        self.qa = self.half // 12
        self.qb = self.qa // 4
        self.buf, self.rcv0, self.rcva, self.rcvb, self.rcvc, self.out = buf, rcv0, rcva, rcvb, rcvc, out
        self.s_snd, self.s_rcv = s_snd, s_rcv
        self.core, self.pos, self.partner, self.along = place
        self.own = self.core * self.half

    def copy(self, k, src, dst, peer):
        return pltpu.make_async_remote_copy(src_ref=src, dst_ref=dst, send_sem=self.s_snd.at[k], recv_sem=self.s_rcv.at[k], device_id=peer, device_id_type=MESH)

    def offset(self, c, depth):
        off = self.own + c * (self.half // 3)
        if depth >= 1:
            off = off + self.qa * self.pos[AXES[c][0]]
        if depth >= 2:
            off = off + self.qb * self.pos[AXES[c][1]]
        return off

    def copies(self, stage):
        out = []
        for d in (1, 3, 2):
            for c in range(3):
                k = 1 + 9 * stage + 3 * (d - 1) + c
                axis = AXES[c][(0, 1, 2, 1, 0)[stage]]
                there, peer = self.along(axis, d)
                if stage == 0:
                    src, dst = self.buf.at[pl.ds(self.offset(c, 0) + self.qa * there, self.qa)], self.rcva.at[c, d - 1]
                elif stage == 1:
                    src, dst = self.buf.at[pl.ds(self.offset(c, 1) + self.qb * there, self.qb)], self.rcvb.at[c, d - 1]
                elif stage == 2:
                    src = dst = self.rcvc.at[c, self.pos[axis]]
                elif stage == 3:
                    src = dst = self.out.at[pl.ds(self.offset(c, 2), self.qb)]
                else:
                    src = dst = self.out.at[pl.ds(self.offset(c, 1), self.qa)]
                out.append(self.copy(k, src, dst, peer))
        return out

    def forwards(self):
        out = []
        for c in range(3):
            for d in range(4):
                off = self.offset(c, 0) + self.qa * lax.rem(self.pos[AXES[c][0]] + 4 - d, 4)
                ref = self.out.at[pl.ds(off, self.qa)]
                out.append(self.copy(46 + 4 * c + d, ref, ref, self.partner))
        return out

    def swap(self):
        other = pl.ds(self.half - self.own, self.half)
        return self.copy(0, self.buf.at[other], self.rcv0, self.partner)

    def run(self, stage):
        if stage == 0:
            self.swap().start()
            return
        if stage == 1:
            self.swap().wait()
            at = pl.ds(self.own, self.half)
            self.buf[at] = self.buf[at] + self.rcv0[...]
        elif stage <= 6:
            for cp in self.copies(stage - 2):
                cp.wait()
        if stage == 2:
            for c in range(3):
                at = pl.ds(self.offset(c, 1), self.qa)
                self.buf[at] = (self.buf[at] + self.rcva[c, 0]) + (self.rcva[c, 1] + self.rcva[c, 2])
        elif stage == 3:
            for c in range(3):
                self.rcvc[c, self.pos[AXES[c][2]]] = (self.buf[pl.ds(self.offset(c, 2), self.qb)] + self.rcvb[c, 0]) + (self.rcvb[c, 1] + self.rcvb[c, 2])
        elif stage == 4:
            for c in range(3):
                self.out[pl.ds(self.offset(c, 2), self.qb)] = ((self.rcvc[c, 0] + self.rcvc[c, 1]) + self.rcvc[c, 2]) + self.rcvc[c, 3]
        if stage <= 5:
            for cp in self.copies(stage - 1):
                cp.start()
        elif stage == 6:
            for cp in self.forwards():
                cp.start()
        else:
            for cp in self.forwards():
                cp.wait()


POINTS = (
    (2, ((0, 0),)), (3, ((1, 0),)), (4, ((2, 0), (0, 1))), (5, ((3, 0), (1, 1))), (6, ((4, 0), (2, 1), (0, 2))),
    (7, ((5, 0), (3, 1), (1, 2))), (7.3, ((6, 0), (4, 1), (2, 2))), (7.6, ((0, 3), (7, 0), (5, 1), (3, 2))),
    (8, ((1, 3), (6, 1), (4, 2))), (9, ((2, 3), (7, 1), (5, 2))), (10, ((3, 3), (6, 2))), (11, ((4, 3), (7, 2))),
    (12, ((5, 3),)), (13, ((6, 3), (7, 3))))


def sweeps_kernel(g_ref, a_ref, q_ref, w_ref, inv_ref, s_ref, rhs_ref, *rest):
    core = lax.axis_index("outer")
    row = lax.axis_index("rows")
    pos = (lax.rem(row, 4), lax.rem(row // 4, 4), row // 16)
    partner = (0, 1 - core, row)

    def along(axis, d):
        there = lax.rem(pos[axis] + d, 4)
        return there, (0, core, row + (there - pos[axis]) * STRIDE[axis])

    barrier = pltpu.get_barrier_semaphore()
    peers = [partner] + [along(axis, d)[1] for axis in range(3) for d in (1, 2, 3)]
    for peer in peers:
        pl.semaphore_signal(barrier, inc=1, device_id=peer, device_id_type=MESH)

    sums = [PanelSum(n, *rest[8 * n:8 * n + 8], (core, pos, partner, along)) for n in range(NP)]
    r = lax.broadcasted_iota(jnp.int32, (NB, NB), 0)
    c = lax.broadcasted_iota(jnp.int32, (NB, NB), 1)
    q_ref[...] = a_ref[...]
    unpack(g_ref, w_ref.at[0])
    for n in range(NP):
        used = 64 * (n + 1)
        if used < SIZES[n]:
            sums[n].buf[used:] = jnp.zeros((SIZES[n] - used, TILE, NB), jnp.float32)

    def gram_panel(n):
        def block(t):
            g = mm_tn(q_ref[:, ds(t, PB)], q_ref[:, n * PB:(n + 1) * PB])
            for i in (0, 1):
                for j in (0, 1):
                    sums[n].buf[pl.ds((4 * t + 2 * i + j) * BT, BT)] = g[i * NB:(i + 1) * NB, j * NB:(j + 1) * NB].reshape(BT, TILE, NB)
        loop(0, n + 1, block)

    def unpack_panel(n):
        def block(t):
            for i in (0, 1):
                for j in (0, 1):
                    w_ref[1, ds(2 * t + i, NB), (2 * n + j) * NB:(2 * n + j + 1) * NB] = sums[n].out[pl.ds((4 * t + 2 * i + j) * BT, BT)].reshape(NB, NB)
        loop(0, n + 1, block)

    def service(point):
        for stage, n in dict(POINTS)[point]:
            if stage == 0:
                gram_panel(n)
                if n == 0:
                    pl.semaphore_wait(barrier, len(peers))
            sums[n].run(stage)
            if stage == 7:
                unpack_panel(n)

    def update(m, s, d, rhs, keep):
        rows = ds(m, PB)
        base = jnp.where(keep, q_ref[rows, ds(d, PB)], 0.0)
        q_ref[rows, ds(d, PB)] = base - mm(q_ref[rows, ds(s, PB)], rhs)

    def solve(m, n):
        q_ref[ds(m, PB), ds(n, PB)] = mm_nt(q_ref[ds(m, PB), ds(n, PB)], inv_ref[n])

    def step(st):
        sw = st // 8
        k = lax.rem(st, 8)
        p = k // 2
        h = lax.rem(k, 2)
        w = w_ref.at[sw]
        q = jnp.maximum(p - 1, 0)
        z = jnp.maximum(p - 2, 0)

        @pl.when(h == 0)
        def _():
            def solved(t):
                w[ds(t, PB), ds(p, PB)] = mm(inv_ref[t], w[ds(t, PB), ds(p, PB)])

                def below(i):
                    w[ds(i, PB), ds(p, PB)] = w[ds(i, PB), ds(p, PB)] - mm_tn(w[ds(t, PB), ds(i, PB)], w[ds(t, PB), ds(p, PB)])
                loop(t + 1, p + 1, below)
            loop(0, p, solved)
            rhs_ref[0] = -inv_ref[q].T
            rhs_ref[1] = w[ds(z, PB), ds(p, PB)]

        @pl.when(h == 1)
        def _():
            rhs_ref[0] = w[ds(q, PB), ds(p, PB)]

        @pl.when(p == 0)
        def _():
            rhs_ref[0] = jnp.zeros((PB, PB), jnp.float32)

        @pl.when(p < 2)
        def _():
            rhs_ref[1] = jnp.zeros((PB, PB), jnp.float32)

        keep = h + (p == 0).astype(jnp.int32) > 0
        dst = jnp.where(h == 0, q, p)
        tasks = [functools.partial(update, m, q, dst, rhs_ref[0], keep) for m in range(4)]
        tasks += [functools.partial(update, 2 * h + m, z, p, rhs_ref[1], True) for m in range(2)]
        rows = ds(k, NB)
        s_ref[:, :NB] = w[rows, rows]
        s_ref[:, NB:] = jnp.where(r == c, 1.0, 0.0).astype(jnp.float32)
        factor_diag(s_ref, tasks)
        w[rows, rows] = jnp.where(c >= r, s_ref[:, :NB], 0.0)
        inv_ref[p, ds(h, NB), ds(h, NB)] = s_ref[:, NB:]

        @pl.when(h == 0)
        def _():
            top, nxt = ds(k, NB), ds(k + 1, NB)
            u01 = mm(inv_ref[p, :NB, :NB], w[top, nxt])
            w[top, nxt] = u01
            w[nxt, nxt] = w[nxt, nxt] - mm_tn(u01, u01)
            w[nxt, top] = jnp.zeros((NB, NB), jnp.float32)

        @pl.when(h == 1)
        def _():
            i0 = inv_ref[p, :NB, :NB]
            i1 = inv_ref[p, NB:, NB:]
            inv_ref[p, NB:, :NB] = -mm(i1, mm_tn(w[ds(k - 1, NB), ds(k, NB)], i0))
            inv_ref[p, :NB, NB:] = jnp.zeros((NB, NB), jnp.float32)

        @pl.when(k == 7)
        def _():
            loop(0, 4, lambda m: update(m, 0, 3, w[0:PB, 3 * PB:], True))

        for point, _ in POINTS:
            if point == int(point):
                @pl.when(st == point)
                def _(point=point):
                    service(point)
                    if point == 7:
                        loop(0, 4, lambda m: solve(m, 3))
                        service(7.3)
                        service(7.6)

    loop(0, 16, step)


def finish_kernel(q_in, w_ref, inv_ref, r_ref, q_ref):
    q_ref[...] = q_in[...]

    def solve(m):
        q_ref[ds(m, PB), 3 * PB:] = mm_nt(q_in[ds(m, PB), 3 * PB:], inv_ref[3])
    loop(0, NP, solve)
    r_ref[...] = jnp.zeros((N, N), jnp.float32)

    def ri(i):
        def rj(j):
            def rk(k):
                r_ref[ds(i, PB), ds(j, PB)] = r_ref[ds(i, PB), ds(j, PB)] + mm(w_ref[1, ds(i, PB), ds(k, PB)], w_ref[0, ds(k, PB), ds(j, PB)])
            loop(i, j + 1, rk)
        loop(i, NP, rj)
    loop(0, NP, ri)


def shape(*dims):
    return jax.ShapeDtypeStruct(dims, jnp.float32)


def sweeps(g, a):
    f32 = jnp.float32
    scratch = [pltpu.VMEM((NB, 2 * NB), f32), pltpu.VMEM((2, PB, PB), f32)]
    for size in SIZES:
        qa, qb = size // 24, size // 96
        scratch += [pltpu.VMEM((size, TILE, NB), f32), pltpu.VMEM((size // 2, TILE, NB), f32), pltpu.VMEM((3, 3, qa, TILE, NB), f32), pltpu.VMEM((3, 3, qb, TILE, NB), f32), pltpu.VMEM((3, 4, qb, TILE, NB), f32), pltpu.VMEM((size, TILE, NB), f32)]
        scratch += [pltpu.SemaphoreType.DMA((COPIES,)), pltpu.SemaphoreType.DMA((COPIES,))]
    return pl.pallas_call(
        sweeps_kernel, out_shape=[shape(N, N), shape(2, N, N), shape(NP, PB, PB)], in_specs=[VM] * 2, out_specs=[VM] * 3, scratch_shapes=scratch,
        compiler_params=pltpu.CompilerParams(vmem_limit_bytes=SWEEP_VMEM, collective_id=1, has_side_effects=True))(g, a)


def finish(q, w, inv):
    return pl.pallas_call(finish_kernel, out_shape=[shape(N, N), shape(N, N)], in_specs=[VM] * 3, out_specs=[VM] * 2, compiler_params=pltpu.CompilerParams(vmem_limit_bytes=FINISH_VMEM))(q, w, inv)


def solution(mesh):
    row_spec = P(("batch", "outer", "rows"), None)

    def group_qr(a_block):
        q, w, inv = sweeps(gram_reduce(a_block, 0), a_block)
        r_block, q_block = finish(q, w, inv)
        return q_block, r_block

    return jax.shard_map(group_qr, mesh=mesh, in_specs=(row_spec,), out_specs=(row_spec, P("batch", None)), check_vma=False)
```

```python
import functools

import jax
import jax.numpy as jnp
from jax import lax
from jax.experimental import pallas as pl
from jax.experimental.pallas import tpu as pltpu
from jax.sharding import PartitionSpec as P

HI = lax.Precision.HIGHEST
N = 1024
NB = 128
SUB = 8


def mm(a, b):
    return lax.dot_general(a, b, (((1,), (0,)), ((), ())), precision=HI, preferred_element_type=jnp.float32)


def mm_tn(a, b):
    return lax.dot_general(a, b, (((0,), (0,)), ((), ())), precision=HI, preferred_element_type=jnp.float32)


def mm_nt(a, b):
    return lax.dot_general(a, b, (((1,), (1,)), ((), ())), precision=HI, preferred_element_type=jnp.float32)


def lane(v, c):
    return jnp.broadcast_to(v[:, c:c + 1], (SUB, NB))


PB = 256
NP = N // PB


def ds(i, n):
    return pl.ds(pl.multiple_of(i * n, n), n)


def loop(lo, hi, body):
    def step(i, carry):
        body(i)
        return carry
    lax.fori_loop(lo, hi, step, 0)


RG = 3


def factor_diag(s_ref, tasks=()):
    groups = NB // SUB
    tasks = list(tasks)
    for g in range(groups):
        base = SUB * g
        left = jnp.stack([jnp.broadcast_to(s_ref[base + i:base + i + 1, :NB], (SUB, NB)) for i in range(SUB)])
        right = jnp.stack([jnp.broadcast_to(s_ref[base + i:base + i + 1, NB:], (SUB, NB)) for i in range(SUB)])
        a = [jnp.stack([lane(left[j], base + i) for i in range(j, SUB)]) for j in range(SUB)]
        inv, u, rows = [], [], []
        for j in range(SUB):
            rs = lax.rsqrt(a[j][0])
            inv.append(rs)
            rl, rr = left[0] * rs, right[0] * rs
            rows.append((rl, rr))
            s_ref[base + j:base + j + 1, :NB] = rl[0:1]
            s_ref[base + j:base + j + 1, NB:] = rr[0:1]
            if j + 1 < SUB:
                uj = a[j][1:] * rs
                u.append(uj)
                for i in range(j + 1, SUB):
                    a[i] = a[i] - uj[i - j - 1:] * uj[i - j - 1]
                left = left[1:] - uj * rl
                right = right[1:] - uj * rr
        for lo in range(g + 1, groups, RG):
            hi = min(lo + RG, groups)
            n = hi - lo
            at = slice(SUB * lo, SUB * hi)
            bl = s_ref[at, :NB].reshape(n, SUB, NB)
            br = s_ref[at, NB:].reshape(n, SUB, NB)
            v = [jnp.broadcast_to(bl[:, :, base + j:base + j + 1], (n, SUB, NB)) for j in range(SUB)]
            for j in range(SUB):
                m = v[j] * inv[j]
                for j2 in range(j + 1, SUB):
                    v[j2] = v[j2] - m * u[j][j2 - j - 1]
                bl = bl - m * rows[j][0]
                br = br - m * rows[j][1]
            s_ref[at, :NB] = bl.reshape(n * SUB, NB)
            s_ref[at, NB:] = br.reshape(n * SUB, NB)
        if g % 2 == 1 and tasks:
            tasks.pop(0)()
    for task in tasks:
        task()


VM = pl.BlockSpec(memory_space=pltpu.VMEM)
SWEEP_VMEM = 30 * 1024 * 1024
FINISH_VMEM = 16 * 1024 * 1024
MESH = pl.DeviceIdType.MESH
TILE = 8
BT = NB // TILE
NBLK = N // NB
AXES = ((0, 1, 2), (1, 2, 0), (2, 0, 1))
STRIDE = (1, 4, 16)


SIZES = (96, 192, 192, 288)
COPIES = 1 + 9 * 5 + 12


class PanelSum:
    def __init__(self, n, buf, rcv0, rcva, rcvb, rcvc, out, s_snd, s_rcv, place):
        self.size = SIZES[n % NP]
        self.half = self.size // 2
        self.qa = self.half // 12
        self.qb = self.qa // 4
        self.buf, self.rcv0, self.rcva, self.rcvb, self.rcvc, self.out = buf, rcv0, rcva, rcvb, rcvc, out
        self.s_snd, self.s_rcv = s_snd, s_rcv
        self.core, self.pos, self.partner, self.near = place
        self.own = self.core * self.half
        self.other = self.half - self.own
        self.offsets = {}
        for c in range(3):
            self.offsets[c, 0] = self.own + c * (self.half // 3)
            self.offsets[c, 1] = self.offsets[c, 0] + self.qa * self.pos[AXES[c][0]]
            self.offsets[c, 2] = self.offsets[c, 1] + self.qb * self.pos[AXES[c][1]]

    def copy(self, k, src, dst, peer):
        return pltpu.make_async_remote_copy(src_ref=src, dst_ref=dst, send_sem=self.s_snd.at[k], recv_sem=self.s_rcv.at[k], device_id=peer, device_id_type=MESH)

    def offset(self, c, depth):
        return self.offsets[c, depth]

    def copies(self, stage):
        out = []
        for d in (1, 3, 2):
            for c in range(3):
                k = 1 + 9 * stage + 3 * (d - 1) + c
                axis = AXES[c][(0, 1, 2, 1, 0)[stage]]
                there, peer = self.near[axis, d]
                if stage == 0:
                    src, dst = self.buf.at[pl.ds(self.offset(c, 0) + self.qa * there, self.qa)], self.rcva.at[c, d - 1]
                elif stage == 1:
                    src, dst = self.buf.at[pl.ds(self.offset(c, 1) + self.qb * there, self.qb)], self.rcvb.at[c, d - 1]
                elif stage == 2:
                    src = dst = self.rcvc.at[c, self.pos[axis]]
                elif stage == 3:
                    src = dst = self.out.at[pl.ds(self.offset(c, 2), self.qb)]
                else:
                    src = dst = self.out.at[pl.ds(self.offset(c, 1), self.qa)]
                out.append(self.copy(k, src, dst, peer))
        return out

    def forwards(self):
        out = []
        for c in range(3):
            for d in range(4):
                axis = AXES[c][0]
                came = self.near[axis, 4 - d][0] if d else self.pos[axis]
                ref = self.out.at[pl.ds(self.offset(c, 0) + self.qa * came, self.qa)]
                out.append(self.copy(46 + 4 * c + d, ref, ref, self.partner))
        return out

    def swap(self):
        other = pl.ds(self.other, self.half)
        return self.copy(0, self.buf.at[other], self.rcv0, self.partner)

    def run(self, stage):
        if stage == 0:
            self.swap().start()
            return
        if stage == 1:
            self.swap().wait()
            at = pl.ds(self.own, self.half)
            self.buf[at] = self.buf[at] + self.rcv0[...]
        elif stage <= 6:
            for cp in self.copies(stage - 2):
                cp.wait()
        if stage == 2:
            for c in range(3):
                at = pl.ds(self.offset(c, 1), self.qa)
                self.buf[at] = (self.buf[at] + self.rcva[c, 0]) + (self.rcva[c, 1] + self.rcva[c, 2])
        elif stage == 3:
            for c in range(3):
                self.rcvc[c, self.pos[AXES[c][2]]] = (self.buf[pl.ds(self.offset(c, 2), self.qb)] + self.rcvb[c, 0]) + (self.rcvb[c, 1] + self.rcvb[c, 2])
        elif stage == 4:
            for c in range(3):
                self.out[pl.ds(self.offset(c, 2), self.qb)] = ((self.rcvc[c, 0] + self.rcvc[c, 1]) + self.rcvc[c, 2]) + self.rcvc[c, 3]
        if stage <= 5:
            for cp in self.copies(stage - 1):
                cp.start()
        elif stage == 6:
            for cp in self.forwards():
                cp.start()
        else:
            for cp in self.forwards():
                cp.wait()


START = (((0, 0),), ((0, 1), (1, 0)), ((0, 2), (2, 0), (1, 1)), ((0, 3), (3, 0), (2, 1), (1, 2)), ((4, 0), (3, 1), (2, 2), (1, 3)), ((5, 0), (4, 1), (3, 2), (2, 3)), ((6, 0), (5, 1), (4, 2), (3, 3)), ((7, 0),))
POINTS = {
    0: ((6, 1), (5, 2), (4, 3)), 1: ((7, 1), (6, 2), (5, 3)), 2: ((0, 4), (7, 2), (6, 3)), 3: ((1, 4), (7, 3)),
    4: ((2, 4), (0, 5)), 5: ((3, 4), (1, 5)), 6: ((4, 4), (2, 5), (0, 6)),
    7: ((5, 4), (3, 5), (1, 6)), 7.3: ((6, 4), (4, 5), (2, 6)), 7.6: ((0, 7), (7, 4), (5, 5), (3, 6)),
    8: ((1, 7), (6, 5), (4, 6)), 9: ((2, 7), (7, 5), (5, 6)), 10: ((3, 7), (6, 6)), 11: ((4, 7), (7, 6)),
    12: ((5, 7),), 13: ((6, 7), (7, 7))}


def sweeps_kernel(a_ref, q_ref, w_ref, inv_ref, s_ref, rhs_ref, *rest):
    core = lax.axis_index("outer")
    row = lax.axis_index("rows")
    pos = (lax.rem(row, 4), lax.rem(row // 4, 4), row // 16)
    partner = (0, 1 - core, row)

    def along(axis, d):
        there = lax.rem(pos[axis] + d, 4)
        return there, (0, core, row + (there - pos[axis]) * STRIDE[axis])

    barrier = pltpu.get_barrier_semaphore()
    near = {(axis, d): along(axis, d) for axis in range(3) for d in (1, 2, 3)}
    peers = [partner] + [peer for _, peer in near.values()]
    for peer in peers:
        pl.semaphore_signal(barrier, inc=1, device_id=peer, device_id_type=MESH)

    sums = [PanelSum(n, *rest[8 * n:8 * n + 8], (core, pos, partner, near)) for n in range(2 * NP)]
    r = lax.broadcasted_iota(jnp.int32, (NB, NB), 0)
    c = lax.broadcasted_iota(jnp.int32, (NB, NB), 1)
    for n in range(2 * NP):
        used = 64 * (n % NP + 1)
        if used < sums[n].size:
            sums[n].buf[used:] = jnp.zeros((sums[n].size - used, TILE, NB), jnp.float32)

    def gram_panel(n):
        ref, p = (a_ref, q_ref)[n // NP], n % NP

        def block(t):
            g = mm_tn(ref[:, ds(t, PB)], ref[:, p * PB:(p + 1) * PB])
            for i in (0, 1):
                for j in (0, 1):
                    sums[n].buf[pl.ds((4 * t + 2 * i + j) * BT, BT)] = g[i * NB:(i + 1) * NB, j * NB:(j + 1) * NB].reshape(BT, TILE, NB)
        loop(0, p + 1, block)

    def unpack_panel(n):
        sw, p = n // NP, n % NP

        def block(t):
            for i in (0, 1):
                for j in (0, 1):
                    w_ref[sw, ds(2 * t + i, NB), (2 * p + j) * NB:(2 * p + j + 1) * NB] = sums[n].out[pl.ds((4 * t + 2 * i + j) * BT, BT)].reshape(NB, NB)
        loop(0, p + 1, block)

    def service(stages):
        for stage, n in stages:
            if stage == 0:
                gram_panel(n)
                if n == 0:
                    pl.semaphore_wait(barrier, len(peers))
            sums[n].run(stage)
            if stage == 7:
                unpack_panel(n)

    def update(m, s, d, rhs, keep):
        rows = ds(m, PB)
        base = jnp.where(keep, q_ref[rows, ds(d, PB)], 0.0)
        q_ref[rows, ds(d, PB)] = base - mm(q_ref[rows, ds(s, PB)], rhs)

    def solve(m, n):
        q_ref[ds(m, PB), ds(n, PB)] = mm_nt(q_ref[ds(m, PB), ds(n, PB)], inv_ref[n])

    def step(st):
        sw = st // 8
        k = lax.rem(st, 8)
        p = k // 2
        h = lax.rem(k, 2)
        w = w_ref.at[sw]
        q = jnp.maximum(p - 1, 0)
        z = jnp.maximum(p - 2, 0)

        @pl.when(h == 0)
        def _():
            for n in range(1, NP):
                @pl.when(p == n)
                def _(n=n):
                    cols = slice(n * PB, (n + 1) * PB)
                    blocks = [w[t * PB:(t + 1) * PB, cols] for t in range(n + 1)]
                    for t in range(n):
                        top = slice(t * PB, (t + 1) * PB)
                        blocks[t] = mm(inv_ref[t], blocks[t])
                        w[top, cols] = blocks[t]
                        for i in range(t + 1, n):
                            blocks[i] = blocks[i] - mm_tn(w[top, i * PB:(i + 1) * PB], blocks[t])
                        blocks[n] = blocks[n] - mm_tn(blocks[t], blocks[t])
                    w[cols, cols] = blocks[n]
            rhs_ref[0] = -inv_ref[q].T
            rhs_ref[1] = w[ds(z, PB), ds(p, PB)]

        @pl.when(h == 1)
        def _():
            rhs_ref[0] = w[ds(q, PB), ds(p, PB)]

        @pl.when(p == 0)
        def _():
            rhs_ref[0] = jnp.zeros((PB, PB), jnp.float32)

        @pl.when(p < 2)
        def _():
            rhs_ref[1] = jnp.zeros((PB, PB), jnp.float32)

        keep = h + (p == 0).astype(jnp.int32) > 0
        dst = jnp.where(h == 0, q, p)
        tasks = [functools.partial(update, m, q, dst, rhs_ref[0], keep) for m in range(4)]
        tasks += [functools.partial(update, 2 * h + m, z, p, rhs_ref[1], True) for m in range(2)]
        rows = ds(k, NB)
        s_ref[:, :NB] = w[rows, rows]
        s_ref[:, NB:] = jnp.where(r == c, 1.0, 0.0).astype(jnp.float32)
        factor_diag(s_ref, tasks)
        w[rows, rows] = jnp.where(c >= r, s_ref[:, :NB], 0.0)
        inv_ref[p, ds(h, NB), ds(h, NB)] = s_ref[:, NB:]

        @pl.when(h == 0)
        def _():
            top, nxt = ds(k, NB), ds(k + 1, NB)
            i0 = inv_ref[p, :NB, :NB]
            u01 = mm(i0, w[top, nxt])
            inv_ref[p, NB:, :NB] = mm_tn(u01, i0)
            w[top, nxt] = u01
            w[nxt, nxt] = w[nxt, nxt] - mm_tn(u01, u01)
            w[nxt, top] = jnp.zeros((NB, NB), jnp.float32)

        @pl.when(h == 1)
        def _():
            inv_ref[p, NB:, :NB] = -mm(inv_ref[p, NB:, NB:], inv_ref[p, NB:, :NB])
            inv_ref[p, :NB, NB:] = jnp.zeros((NB, NB), jnp.float32)

        @pl.when(k == 7)
        def _():
            loop(0, 4, lambda m: update(m, 0, 3, w[0:PB, 3 * PB:], True))

        for point in POINTS:
            if point == int(point):
                @pl.when(st == point)
                def _(point=point):
                    service(POINTS[point])
                    if point == 7:
                        loop(0, 4, lambda m: solve(m, 3))
                        service(POINTS[7.3])
                        service(POINTS[7.6])

    for n, stages in enumerate(START):
        if n == 4:
            q_ref[...] = a_ref[...]
        service(stages)
    loop(0, 16, step)


def finish_kernel(q_in, w_ref, inv_ref, r_hbm, q_hbm, r_ref, q_ref, sems):
    ready = pltpu.make_async_copy(q_in.at[:, :3 * PB], q_hbm.at[:, :3 * PB], sems.at[0])
    ready.start()

    def solve(m):
        q_ref[ds(m, PB), :] = mm_nt(q_in[ds(m, PB), 3 * PB:], inv_ref[3])
    loop(0, NP, solve)
    rest = pltpu.make_async_copy(q_ref, q_hbm.at[:, 3 * PB:], sems.at[1])
    rest.start()
    r_ref[...] = jnp.zeros((N, N), jnp.float32)
    copies = [ready, rest]
    for i in range(NP):
        for j in range(i, NP):
            span = slice(i * PB, (j + 1) * PB)
            r_ref[i * PB:(i + 1) * PB, j * PB:(j + 1) * PB] = mm(w_ref[1, i * PB:(i + 1) * PB, span], w_ref[0, span, j * PB:(j + 1) * PB])
        copies.append(pltpu.make_async_copy(r_ref.at[i * PB:(i + 1) * PB], r_hbm.at[i * PB:(i + 1) * PB], sems.at[2 + i]))
        copies[-1].start()
    for cp in copies:
        cp.wait()


def shape(*dims):
    return jax.ShapeDtypeStruct(dims, jnp.float32)


def sweeps(a):
    f32 = jnp.float32
    scratch = [pltpu.VMEM((NB, 2 * NB), f32), pltpu.VMEM((2, PB, PB), f32)]
    for size in SIZES * 2:
        qa, qb = size // 24, size // 96
        scratch += [pltpu.VMEM((size, TILE, NB), f32), pltpu.VMEM((size // 2, TILE, NB), f32), pltpu.VMEM((3, 3, qa, TILE, NB), f32), pltpu.VMEM((3, 3, qb, TILE, NB), f32), pltpu.VMEM((3, 4, qb, TILE, NB), f32), pltpu.VMEM((size, TILE, NB), f32)]
        scratch += [pltpu.SemaphoreType.DMA((COPIES,)), pltpu.SemaphoreType.DMA((COPIES,))]
    return pl.pallas_call(
        sweeps_kernel, out_shape=[shape(N, N), shape(2, N, N), shape(NP, PB, PB)], in_specs=[VM], out_specs=[VM] * 3, scratch_shapes=scratch,
        compiler_params=pltpu.CompilerParams(vmem_limit_bytes=SWEEP_VMEM, collective_id=0, has_side_effects=True))(a)


def finish(q, w, inv):
    return pl.pallas_call(finish_kernel, out_shape=[shape(N, N), shape(N, N)], in_specs=[VM] * 3, out_specs=[pl.BlockSpec(memory_space=pl.ANY)] * 2, scratch_shapes=[pltpu.VMEM((N, N), jnp.float32), pltpu.VMEM((N, PB), jnp.float32), pltpu.SemaphoreType.DMA((2 + NP,))], compiler_params=pltpu.CompilerParams(vmem_limit_bytes=FINISH_VMEM))(q, w, inv)


def solution(mesh):
    row_spec = P(("batch", "outer", "rows"), None)

    def group_qr(a_block):
        q, w, inv = sweeps(a_block)
        r_block, q_block = finish(q, w, inv)
        return q_block, r_block

    return jax.shard_map(group_qr, mesh=mesh, in_specs=(row_spec,), out_specs=(row_spec, P("batch", None)), check_vma=False)
```

```python
import functools

import jax
import jax.numpy as jnp
from jax import lax
from jax.experimental import pallas as pl
from jax.experimental.pallas import tpu as pltpu
from jax.sharding import PartitionSpec as P

HI = lax.Precision.HIGHEST
N = 1024
NB = 128
SUB = 8


def mm(a, b):
    return lax.dot_general(a, b, (((1,), (0,)), ((), ())), precision=HI, preferred_element_type=jnp.float32)


def mm_tn(a, b):
    return lax.dot_general(a, b, (((0,), (0,)), ((), ())), precision=HI, preferred_element_type=jnp.float32)


def mm_nt(a, b):
    return lax.dot_general(a, b, (((1,), (1,)), ((), ())), precision=HI, preferred_element_type=jnp.float32)


def lane(v, c):
    return jnp.broadcast_to(v[:, c:c + 1], (SUB, NB))


PB = 256
NP = N // PB


def ds(i, n):
    return pl.ds(pl.multiple_of(i * n, n), n)


def loop(lo, hi, body):
    def step(i, carry):
        body(i)
        return carry
    lax.fori_loop(lo, hi, step, 0)


RG = 3


def factor_diag(s_ref, tasks=()):
    groups = NB // SUB
    tasks = list(tasks)
    for g in range(groups):
        base = SUB * g
        left = jnp.stack([jnp.broadcast_to(s_ref[base + i:base + i + 1, :NB], (SUB, NB)) for i in range(SUB)])
        right = jnp.stack([jnp.broadcast_to(s_ref[base + i:base + i + 1, NB:], (SUB, NB)) for i in range(SUB)])
        a = [jnp.stack([lane(left[j], base + i) for i in range(j, SUB)]) for j in range(SUB)]
        inv, u, rows = [], [], []
        for j in range(SUB):
            rs = lax.rsqrt(a[j][0])
            inv.append(rs)
            rl, rr = left[0] * rs, right[0] * rs
            rows.append((rl, rr))
            s_ref[base + j:base + j + 1, :NB] = rl[0:1]
            s_ref[base + j:base + j + 1, NB:] = rr[0:1]
            if j + 1 < SUB:
                uj = a[j][1:] * rs
                u.append(uj)
                for i in range(j + 1, SUB):
                    a[i] = a[i] - uj[i - j - 1:] * uj[i - j - 1]
                left = left[1:] - uj * rl
                right = right[1:] - uj * rr
        for lo in range(g + 1, groups, RG):
            hi = min(lo + RG, groups)
            n = hi - lo
            at = slice(SUB * lo, SUB * hi)
            bl = s_ref[at, :NB].reshape(n, SUB, NB)
            br = s_ref[at, NB:].reshape(n, SUB, NB)
            v = [jnp.broadcast_to(bl[:, :, base + j:base + j + 1], (n, SUB, NB)) for j in range(SUB)]
            for j in range(SUB):
                m = v[j] * inv[j]
                for j2 in range(j + 1, SUB):
                    v[j2] = v[j2] - m * u[j][j2 - j - 1]
                bl = bl - m * rows[j][0]
                br = br - m * rows[j][1]
            s_ref[at, :NB] = bl.reshape(n * SUB, NB)
            s_ref[at, NB:] = br.reshape(n * SUB, NB)
        if g % 2 == 1 and tasks:
            tasks.pop(0)()
    for task in tasks:
        task()


VM = pl.BlockSpec(memory_space=pltpu.VMEM)
SWEEP_VMEM = 30 * 1024 * 1024
FINISH_VMEM = 16 * 1024 * 1024
MESH = pl.DeviceIdType.MESH
TILE = 8
BT = NB // TILE
NBLK = N // NB
AXES = ((0, 1, 2), (1, 2, 0), (2, 0, 1))
STRIDE = (1, 4, 16)


SIZES = (96, 192, 192, 288)
COPIES = 1 + 9 * 5 + 12


class PanelSum:
    def __init__(self, n, buf, rcv0, rcva, rcvb, rcvc, out, s_snd, s_rcv, place):
        self.size = SIZES[n % NP]
        self.half = self.size // 2
        self.qa = self.half // 12
        self.qb = self.qa // 4
        self.flat = n % NP == 0
        self.buf, self.rcv0, self.rcva, self.rcvb, self.rcvc, self.out = buf, rcv0, rcva, rcvb, rcvc, out
        self.s_snd, self.s_rcv = s_snd, s_rcv
        self.core, self.pos, self.partner, self.near = place
        self.own = self.core * self.half
        self.other = self.half - self.own
        self.offsets = {}
        for c in range(3):
            self.offsets[c, 0] = self.own + c * (self.half // 3)
            self.offsets[c, 1] = self.offsets[c, 0] + self.qa * self.pos[AXES[c][0]]
            self.offsets[c, 2] = self.offsets[c, 1] + self.qb * self.pos[AXES[c][1]]

    def copy(self, k, src, dst, peer):
        return pltpu.make_async_remote_copy(src_ref=src, dst_ref=dst, send_sem=self.s_snd.at[k], recv_sem=self.s_rcv.at[k], device_id=peer, device_id_type=MESH)

    def offset(self, c, depth):
        return self.offsets[c, depth]

    def copies(self, stage):
        out = []
        for d in (1, 3, 2):
            for c in range(3):
                k = 1 + 9 * stage + 3 * (d - 1) + c
                axis = AXES[c][(0, 1, 2, 1, 0)[stage]]
                there, peer = self.near[axis, d]
                if stage == 0:
                    src, dst = self.buf.at[pl.ds(self.offset(c, 0) + self.qa * there, self.qa)], self.rcva.at[c, d - 1]
                elif stage == 1 and self.flat:
                    src = dst = self.rcvb.at[c, self.pos[axis]]
                elif stage == 1:
                    src, dst = self.buf.at[pl.ds(self.offset(c, 1) + self.qb * there, self.qb)], self.rcvb.at[c, d - 1]
                elif stage == 2:
                    src = dst = self.rcvc.at[c, self.pos[axis]]
                elif stage == 3:
                    src = dst = self.out.at[pl.ds(self.offset(c, 2), self.qb)]
                else:
                    src = dst = self.out.at[pl.ds(self.offset(c, 1), self.qa)]
                out.append(self.copy(k, src, dst, peer))
        return out

    def forwards(self):
        out = []
        for c in range(3):
            for d in range(4):
                axis = AXES[c][0]
                came = self.near[axis, 4 - d][0] if d else self.pos[axis]
                ref = self.out.at[pl.ds(self.offset(c, 0) + self.qa * came, self.qa)]
                out.append(self.copy(46 + 4 * c + d, ref, ref, self.partner))
        return out

    def swap(self):
        other = pl.ds(self.other, self.half)
        return self.copy(0, self.buf.at[other], self.rcv0, self.partner)

    def in_order(self, ref, c):
        return ((ref[c, 0] + ref[c, 1]) + ref[c, 2]) + ref[c, 3]

    def run(self, stage):
        if stage == 0:
            self.swap().start()
            return
        if stage == 1:
            self.swap().wait()
            at = pl.ds(self.own, self.half)
            self.buf[at] = self.buf[at] + self.rcv0[...]
        elif stage <= 6:
            for cp in self.copies(stage - 2):
                cp.wait()
        if stage == 2:
            for c in range(3):
                at = pl.ds(self.offset(c, 1), self.qa)
                total = (self.buf[at] + self.rcva[c, 0]) + (self.rcva[c, 1] + self.rcva[c, 2])
                if self.flat:
                    self.rcvb[c, self.pos[AXES[c][1]]] = total
                else:
                    self.buf[at] = total
        elif stage == 3 and self.flat:
            for c in range(3):
                self.rcvc[c, self.pos[AXES[c][2]]] = self.in_order(self.rcvb, c)
        elif stage == 3:
            for c in range(3):
                self.rcvc[c, self.pos[AXES[c][2]]] = (self.buf[pl.ds(self.offset(c, 2), self.qb)] + self.rcvb[c, 0]) + (self.rcvb[c, 1] + self.rcvb[c, 2])
        elif stage == 4:
            for c in range(3):
                at = pl.ds(self.offset(c, 1), self.qa) if self.flat else pl.ds(self.offset(c, 2), self.qb)
                self.out[at] = self.in_order(self.rcvc, c)
        if stage <= 5:
            for cp in self.copies(4 if self.flat and stage == 4 else stage - 1):
                cp.start()
        elif stage == 6:
            for cp in self.forwards():
                cp.start()
        else:
            for cp in self.forwards():
                cp.wait()


START = (
    ((0, 0, 1), ((0, 0),)), ((1, 0, 2), ((1, 0), (0, 1))), ((2, 0, 3), ((2, 0), (0, 2), (1, 1))),
    ((3, 0, 2), ((3, 0), (2, 1), (1, 2))), ((3, 2, 4), ((0, 3), (4, 0), (3, 1), (2, 2))),
    (None, ((6, 0), (4, 1), (3, 2), (1, 3))), (None, ((7, 0), (5, 1))))
POINTS = {
    0: ((6, 1), (4, 2), (2, 3)), 1: ((7, 1), (5, 2), (3, 3)), 2: ((0, 4), (6, 2), (4, 3)), 3: ((1, 4), (7, 2), (5, 3)),
    4: ((2, 4), (0, 5), (6, 3)), 5: ((3, 4), (1, 5), (7, 3)), 6: ((4, 4), (2, 5), (0, 6)),
    7: ((6, 4), (3, 5), (1, 6)), 7.3: ((7, 4), (4, 5), (2, 6)), 7.6: ((0, 7), (5, 5), (3, 6)),
    8: ((1, 7), (6, 5), (4, 6)), 9: ((2, 7), (7, 5), (5, 6)), 10: ((3, 7), (6, 6)), 11: ((4, 7), (7, 6)),
    12: ((5, 7),), 13: ((6, 7), (7, 7))}


def sweeps_kernel(a_ref, q_ref, w_ref, inv_ref, s_ref, rhs_ref, s_in, *rest):
    core = lax.axis_index("outer")
    row = lax.axis_index("rows")
    pos = (lax.rem(row, 4), lax.rem(row // 4, 4), row // 16)
    partner = (0, 1 - core, row)

    def along(axis, d):
        there = lax.rem(pos[axis] + d, 4)
        return there, (0, core, row + (there - pos[axis]) * STRIDE[axis])

    fetch = [pltpu.make_async_copy(a_ref.at[:, n * PB:(n + 1) * PB], q_ref.at[:, n * PB:(n + 1) * PB], s_in.at[n]) for n in range(NP)]
    for cp in fetch:
        cp.start()

    barrier = pltpu.get_barrier_semaphore()
    near = {(axis, d): along(axis, d) for axis in range(3) for d in (1, 2, 3)}
    peers = [partner] + [peer for _, peer in near.values()]
    for peer in peers:
        pl.semaphore_signal(barrier, inc=1, device_id=peer, device_id_type=MESH)

    sums = [PanelSum(n, *rest[8 * n:8 * n + 8], (core, pos, partner, near)) for n in range(2 * NP)]
    r = lax.broadcasted_iota(jnp.int32, (NB, NB), 0)
    c = lax.broadcasted_iota(jnp.int32, (NB, NB), 1)
    for n in range(2 * NP):
        used = 64 * (n % NP + 1)
        if used < sums[n].size:
            sums[n].buf[used:] = jnp.zeros((sums[n].size - used, TILE, NB), jnp.float32)

    def gram_panel(n, lo, hi):
        p = n % NP

        def block(t):
            g = mm_tn(q_ref[:, ds(t, PB)], q_ref[:, p * PB:(p + 1) * PB])
            for i in (0, 1):
                for j in (0, 1):
                    sums[n].buf[pl.ds((4 * t + 2 * i + j) * BT, BT)] = g[i * NB:(i + 1) * NB, j * NB:(j + 1) * NB].reshape(BT, TILE, NB)
        loop(lo, hi, block)

    def unpack_panel(n):
        sw, p = n // NP, n % NP

        def block(t):
            for i in (0, 1):
                for j in (0, 1):
                    w_ref[sw, ds(2 * t + i, NB), (2 * p + j) * NB:(2 * p + j + 1) * NB] = sums[n].out[pl.ds((4 * t + 2 * i + j) * BT, BT)].reshape(NB, NB)
        loop(0, p + 1, block)

    def service(stages):
        for stage, n in stages:
            if stage == 0 and n >= NP:
                gram_panel(n, 0, n - NP + 1)
            sums[n].run(stage)
            if stage == 7:
                unpack_panel(n)

    def update(m, s, d, rhs, keep):
        rows = ds(m, PB)
        base = jnp.where(keep, q_ref[rows, ds(d, PB)], 0.0)
        q_ref[rows, ds(d, PB)] = base - mm(q_ref[rows, ds(s, PB)], rhs)

    def solve(m, n):
        q_ref[ds(m, PB), ds(n, PB)] = mm_nt(q_ref[ds(m, PB), ds(n, PB)], inv_ref[n])

    def step(st):
        sw = st // 8
        k = lax.rem(st, 8)
        p = k // 2
        h = lax.rem(k, 2)
        w = w_ref.at[sw]
        q = jnp.maximum(p - 1, 0)
        z = jnp.maximum(p - 2, 0)

        @pl.when(h == 0)
        def _():
            for n in range(1, NP):
                @pl.when(p == n)
                def _(n=n):
                    cols = slice(n * PB, (n + 1) * PB)
                    blocks = [w[t * PB:(t + 1) * PB, cols] for t in range(n + 1)]
                    for t in range(n):
                        top = slice(t * PB, (t + 1) * PB)
                        blocks[t] = mm(inv_ref[t], blocks[t])
                        w[top, cols] = blocks[t]
                        for i in range(t + 1, n):
                            blocks[i] = blocks[i] - mm_tn(w[top, i * PB:(i + 1) * PB], blocks[t])
                        blocks[n] = blocks[n] - mm_tn(blocks[t], blocks[t])
                    w[cols, cols] = blocks[n]
                    rhs_ref[0] = -inv_ref[n - 1].T
                    rhs_ref[1] = blocks[n - 2] if n > 1 else jnp.zeros((PB, PB), jnp.float32)
            @pl.when(p == 0)
            def _():
                rhs_ref[...] = jnp.zeros((2, PB, PB), jnp.float32)

        @pl.when(h * p > 0)
        def _():
            rhs_ref[0] = w[ds(q, PB), ds(p, PB)]

        keep = h + (p == 0).astype(jnp.int32) > 0
        dst = jnp.where(h == 0, q, p)
        tasks = [functools.partial(update, m, q, dst, rhs_ref[0], keep) for m in range(4)]
        tasks += [functools.partial(update, 2 * h + m, z, p, rhs_ref[1], True) for m in range(2)]
        rows = ds(k, NB)
        s_ref[:, :NB] = w[rows, rows]
        s_ref[:, NB:] = jnp.where(r == c, 1.0, 0.0).astype(jnp.float32)
        factor_diag(s_ref, tasks)
        w[rows, rows] = jnp.where(c >= r, s_ref[:, :NB], 0.0)
        inv_ref[p, ds(h, NB), ds(h, NB)] = s_ref[:, NB:]

        @pl.when(h == 0)
        def _():
            top, nxt = ds(k, NB), ds(k + 1, NB)
            i0 = inv_ref[p, :NB, :NB]
            u01 = mm(i0, w[top, nxt])
            inv_ref[p, NB:, :NB] = mm_tn(u01, i0)
            w[top, nxt] = u01
            w[nxt, nxt] = w[nxt, nxt] - mm_tn(u01, u01)
            w[nxt, top] = jnp.zeros((NB, NB), jnp.float32)

        @pl.when(h == 1)
        def _():
            inv_ref[p, NB:, :NB] = -mm(inv_ref[p, NB:, NB:], inv_ref[p, NB:, :NB])
            inv_ref[p, :NB, NB:] = jnp.zeros((NB, NB), jnp.float32)

        @pl.when(k == 7)
        def _():
            loop(0, 2, lambda m: (update(2 * m, 0, 3, w[0:PB, 3 * PB:], True), update(2 * m + 1, 0, 3, w[0:PB, 3 * PB:], True)))

        for point in POINTS:
            if point == int(point):
                @pl.when(st == point)
                def _(point=point):
                    service(POINTS[point])
                    if point == 7:
                        loop(0, 2, lambda m: (solve(2 * m, 3), solve(2 * m + 1, 3)))
                        service(POINTS[7.3])
                        service(POINTS[7.6])

    for gram, stages in START:
        if gram:
            if gram[1] == 0:
                fetch[gram[0]].wait()
            gram_panel(*gram)
        if gram == (0, 0, 1):
            pl.semaphore_wait(barrier, len(peers))
        service(stages)
    loop(0, 16, step)


def finish_kernel(q_in, w_ref, inv_ref, r_hbm, q_hbm, r_ref, q_ref, sems):
    ready = pltpu.make_async_copy(q_in.at[:, :3 * PB], q_hbm.at[:, :3 * PB], sems.at[0])
    ready.start()

    def solve(m):
        q_ref[ds(m, PB), :] = mm_nt(q_in[ds(m, PB), 3 * PB:], inv_ref[3])
    loop(0, 2, lambda m: (solve(2 * m), solve(2 * m + 1)))
    rest = pltpu.make_async_copy(q_ref, q_hbm.at[:, 3 * PB:], sems.at[1])
    rest.start()
    r_ref[...] = jnp.zeros((N, N), jnp.float32)
    copies = [ready, rest]
    for i in range(NP):
        for j in range(i, NP):
            span = slice(i * PB, (j + 1) * PB)
            r_ref[i * PB:(i + 1) * PB, j * PB:(j + 1) * PB] = mm(w_ref[1, i * PB:(i + 1) * PB, span], w_ref[0, span, j * PB:(j + 1) * PB])
        copies.append(pltpu.make_async_copy(r_ref.at[i * PB:(i + 1) * PB], r_hbm.at[i * PB:(i + 1) * PB], sems.at[2 + i]))
        copies[-1].start()
    for cp in copies:
        cp.wait()


def shape(*dims):
    return jax.ShapeDtypeStruct(dims, jnp.float32)


def sweeps(a):
    f32 = jnp.float32
    scratch = [pltpu.VMEM((NB, 2 * NB), f32), pltpu.VMEM((2, PB, PB), f32), pltpu.SemaphoreType.DMA((NP,))]
    for n, size in enumerate(SIZES * 2):
        qa, qb = size // 24, size // 96
        late = qa if n % NP == 0 else qb
        scratch += [pltpu.VMEM((size, TILE, NB), f32), pltpu.VMEM((size // 2, TILE, NB), f32), pltpu.VMEM((3, 3, qa, TILE, NB), f32), pltpu.VMEM((3, 4, late, TILE, NB), f32), pltpu.VMEM((3, 4, late, TILE, NB), f32), pltpu.VMEM((size, TILE, NB), f32)]
        scratch += [pltpu.SemaphoreType.DMA((COPIES,)), pltpu.SemaphoreType.DMA((COPIES,))]
    return pl.pallas_call(
        sweeps_kernel, out_shape=[shape(N, N), shape(2, N, N), shape(NP, PB, PB)], in_specs=[pl.BlockSpec(memory_space=pltpu.HBM)], out_specs=[VM] * 3, scratch_shapes=scratch,
        compiler_params=pltpu.CompilerParams(vmem_limit_bytes=SWEEP_VMEM, collective_id=0, has_side_effects=True))(a)


def finish(q, w, inv):
    return pl.pallas_call(finish_kernel, out_shape=[shape(N, N), shape(N, N)], in_specs=[VM] * 3, out_specs=[pl.BlockSpec(memory_space=pl.ANY)] * 2, scratch_shapes=[pltpu.VMEM((N, N), jnp.float32), pltpu.VMEM((N, PB), jnp.float32), pltpu.SemaphoreType.DMA((2 + NP,))], compiler_params=pltpu.CompilerParams(vmem_limit_bytes=FINISH_VMEM))(q, w, inv)


def solution(mesh):
    row_spec = P(("batch", "outer", "rows"), None)

    def group_qr(a_block):
        q, w, inv = sweeps(a_block)
        r_block, q_block = finish(q, w, inv)
        return q_block, r_block

    return jax.shard_map(group_qr, mesh=mesh, in_specs=(row_spec,), out_specs=(row_spec, P("batch", None)), check_vma=False)
```
